512 devices in a mesh: mem: 16 (over z_hi, y, core), lat: 4 (over x), lon: 8 (over z_lo).
Axes of the slice: x: 4, y: 4, z: 16 (z_hi: 2, z_lo: 8; z = z_hi * 8 + z_lo), core: 2. Of those that a mesh axis runs over, the one named last changes fastest.
Arguments:
- perturbation: bfloat16 [64, 64, 128, 1024], P('mem', None, 'lat', 'lon'), may hold values from -6 to 6
- control: bfloat16 [64, 16, 128, 1024], P('mem', None, 'lat', 'lon'), may hold values from -6 to 6
- filter_length: float32 [16], replicated, may hold values from 20 to 2000
- modes: float32 [64, 16], replicated, may hold values from -1.5 to 1.5
- obs_weights: bfloat16 [16384, 64], P(('lat', 'lon')), may hold values from -1.5 to 1.5
- innovation: float32 [16384], P(('lat', 'lon')), may hold values from -6 to 6
- obs_tile: int32 [16384, 1], P(('lat', 'lon')), may hold values from 0 to 31; in each aligned block of 512 rows (0 to 511, 512 to 1023, ...) at most 32 rows name the same one
- obs_column: int32 [16384], P(('lat', 'lon')), may hold values from 0 to 16383
- obs_count: int32 [32], P(('lat', 'lon')), may hold values from 64 to 512, as said below
Outputs:
- increment: float32 [64, 128, 1024], P('mem', 'lat', 'lon')
- departures: float32 [16384], P(('lat', 'lon'))
The draws below stay inside these ranges and needn't reach their ends.
Inputs may be any that keep to these rules, and one draw needn't show every extreme that they name: obs_tile names each tile for at most 32 of the 512 slots of one tile, a bound that some block reaches of them. `obs_count`: some tile has all 512 slots live.
All inputs are finite; a program needn't handle non-finite values.
Results may differ from the reference program's by a relative error of at most 0.0003.
Values sent between devices are 32-bit elements; how exact they have to be, the bound alone decides.
A program may use at most 64 MiB of HBM per device.

```python
import math
import jax
import jax.numpy as jnp
import numpy as np
from jax import lax

CX = 32
CY = 128
LEV = 64
MODES = 16
OBS_DEV = 512
TILES = 32
CAP = 32
MEMBERS = 64
NX = 128
NY = 1024
OBS = 16384
N_LAT = 4
N_LON = 8


def draw_obs_count(key, part):
    first, second = jax.random.split(jax.random.fold_in(key, 11))
    counts = jax.random.randint(first, (TILES,), OBS_DEV // 8, OBS_DEV + 1)
    chosen = jax.random.randint(second, (), 0, TILES)
    return counts.at[chosen].set(OBS_DEV).astype(jnp.int32)


def place_ends(values, rng, least, high):
    longest = values.shape.index(max(values.shape))
    spots = []
    for shift in (0, 1):
        where = [jax.random.randint(jax.random.fold_in(rng, axis), (), 0, length) for axis, length in enumerate(values.shape)]
        where[longest] = (where[longest] + shift) % values.shape[longest]
        spots.append(tuple(where))
    return values.at[spots[0]].set(least).at[spots[1]].set(high)


def block_scale(own_key, dims, shards, low, largest):
    def one(axis_at, shards_of):
        heights = jax.random.uniform(jax.random.fold_in(jax.random.fold_in(own_key, 6), axis_at), (shards_of,), jnp.float32, low / len(shards), largest / len(shards))
        return jnp.repeat(jnp.exp(heights), dims[axis_at] // shards_of).reshape((-1,) + (1,) * (len(dims) - axis_at - 1))

    factor_of = one(*shards[0])
    for cut in shards[1:]:
        factor_of = factor_of * one(*cut)
    return factor_of


def deal_out(own_key, own, number, rows, amount, top, reach, skew):
    order = jax.random.permutation(own_key, amount)
    crowded, ordinary = load_shares(amount, rows * top, reach, skew, True), load_shares(amount, rows * top, reach, skew, False)
    places = jnp.arange(amount)

    def named(sizes, offset_by):
        used = int((sizes > 0).sum())
        fixed = max(1, used // 4)
        passed = fixed + (places - fixed + offset_by * (used - fixed)) % max(1, amount - fixed)
        return jnp.zeros((amount,), jnp.int32).at[order[jnp.where(places < fixed, places, passed)]].set(jnp.asarray(sizes, jnp.int32))

    sizes = jnp.where(number % 4 == 0, named(crowded, number // 4), named(ordinary, number - number // 4 - 1))
    mixed = jax.random.permutation(jax.random.fold_in(own, 3), amount)
    giver, taker = mixed[0:amount // 2 * 2:2], mixed[1:amount // 2 * 2:2]
    margin = jnp.minimum(sizes[giver] - 1, reach - sizes[taker]) // 2
    margin = jnp.where((giver == order[0]) | (taker == order[0]) | (sizes[taker] == 0), 0, jnp.maximum(margin, 0))
    passed = jax.random.randint(jax.random.fold_in(own, 4), (amount // 2,), 0, 1 << 20) % (margin + 1)
    sizes = sizes.at[giver].add(-passed).at[taker].add(passed)
    labels = jnp.searchsorted(jnp.cumsum(sizes), jnp.arange(rows * top), side="right").astype(jnp.int32)
    listing = labels.reshape(top, rows).T
    listing = listing[jax.random.permutation(jax.random.fold_in(own, 1), rows)]
    offset_by = jax.random.randint(jax.random.fold_in(own, 2), (rows, 1), 0, top)
    return jnp.take_along_axis(listing, (jnp.arange(top)[None, :] + offset_by) % top, axis=1)


def load_shares(number_of, total, reach, lean, full):
    portions = [(1 << 20) // math.isqrt(rank ** lean) + 1 for rank in range(1, number_of + 1)]
    largest = reach if full else min(reach, max(-(-total // number_of), total * portions[0] // sum(portions)))
    least = 1 if total - largest >= number_of - 1 else 0
    holding, spare = [largest] + [least] * (number_of - 1), total - largest - least * (number_of - 1)
    while spare > 0:
        movable = [i for i in range(1, number_of) if holding[i] < largest] or [i for i in range(1, number_of) if holding[i] < reach]
        whole, left = sum([portions[i] for i in movable]), spare
        for i in movable:
            more = min(reach - holding[i], max(1, left * portions[i] // whole), spare)
            holding[i] = holding[i] + more
            spare = spare - more
    return np.array(holding)


def normal_values(stream_key, dims, width, limit, cuts=(), kind=jnp.bfloat16):
    array = jax.random.normal(stream_key, dims, jnp.float32) * width
    if len(cuts) > 0:
        array = block_scale(stream_key, dims, cuts, -0.22, 0.18) * array
    return jnp.clip(array, min=-limit, max=limit).astype(kind)


def setup_inputs(seed: int = 0) -> dict:
    keys = jax.random.split(jax.random.key(seed), 10)
    perturbation = normal_values(keys[0], (MEMBERS, LEV, NX, NY), 1.0, 6.0, ((0, 16), (2, 4), (3, 8)))
    control = normal_values(keys[1], (MEMBERS, MODES, NX, NY), 1.0, 6.0, ((0, 16), (2, 4), (3, 8)))
    filter_length = jnp.clip(jnp.exp(jax.random.uniform(keys[2], (MODES,), jnp.float32, math.log(20.0), math.log(2000.0))), 20.0, 2000.0)
    modes = normal_values(keys[3], (LEV, MODES), MODES ** -0.5, 1.5, (), jnp.float32)
    obs_weights = normal_values(keys[4], (OBS, LEV), 0.25, 1.5, ((0, 32),))
    innovation = normal_values(keys[5], (OBS,), 1.0, 6.0, ((0, 32),), jnp.float32)
    obs_tile_keys = jax.random.split(jax.random.fold_in(keys[6], 1), OBS // OBS_DEV)
    obs_tile_turns = jax.random.permutation(jax.random.fold_in(keys[6], 3), OBS // OBS_DEV)
    obs_tile = jax.vmap(lambda own, number: deal_out(jax.random.fold_in(keys[6], 2), own, number, OBS_DEV, TILES, 1, CAP, 2))(obs_tile_keys, obs_tile_turns).reshape((OBS, 1))
    obs_column = place_ends(jax.random.randint(keys[7], (OBS,), 0, 4 * CX * CY), jax.random.fold_in(keys[7], 1), 0, (4 * CX * CY) - 1).astype(jnp.int32)
    obs_count = draw_obs_count(jax.random.fold_in(keys[9], 71), 0)
    return {"perturbation": perturbation, "control": control, "filter_length": filter_length, "modes": modes, "obs_weights": obs_weights, "innovation": innovation, "obs_tile": obs_tile, "obs_column": obs_column, "obs_count": obs_count}


def sweep(field, rate, axis, backward):
    moved = jnp.moveaxis(field, axis, 0)
    decay = rate[:, None]

    def advance(carry, row):
        fresh = decay * carry + (1.0 - decay) * row
        return (fresh, fresh)
    _, result = lax.scan(advance, jnp.zeros_like(moved[0]), moved, reverse=backward)
    return jnp.moveaxis(result, 0, axis)

def reference(perturbation, control, filter_length, modes, obs_weights, innovation, obs_tile, obs_column, obs_count):
    rate = jnp.exp(-1.0 / filter_length)
    boost = (1.0 + rate) / (1.0 - rate)
    members = perturbation.shape[0]

    def member_step(total, pieces):
        member_pert, member_control = pieces
        field = member_control.astype(jnp.float32) * boost[:, None, None]
        field = sweep(field, rate, 1, False)
        field = sweep(field, rate, 1, True)
        field = sweep(field, rate, 2, False)
        field = sweep(field, rate, 2, True)
        profile = jnp.einsum('zk,kxy->zxy', modes, field, precision=lax.Precision.HIGHEST)
        return (total + member_pert.astype(jnp.float32) * profile, None)
    start = jnp.zeros(perturbation.shape[1:], jnp.float32)
    summed, _ = lax.scan(member_step, start, (perturbation, control))
    increment = summed * (1.0 / math.sqrt(members - 1))
    tile_rows = NX // N_LAT
    tile_cols = NY // N_LON
    target = obs_tile[:, 0]
    fine_row = target // N_LON * 2 * tile_rows + obs_column // (2 * tile_cols)
    fine_col = target % N_LON * 2 * tile_cols + obs_column % (2 * tile_cols)
    padded = jnp.pad(increment, ((0, 0), (1, 1), (1, 1)))
    near_row = fine_row // 2 + 1
    far_row = near_row + 2 * (fine_row % 2) - 1
    near_col = fine_col // 2 + 1
    far_col = near_col + 2 * (fine_col % 2) - 1
    blend = 0.5625 * padded[:, near_row, near_col] + 0.1875 * padded[:, far_row, near_col] + 0.1875 * padded[:, near_row, far_col] + 0.0625 * padded[:, far_row, far_col]
    equivalent = lax.optimization_barrier(jnp.sum(obs_weights.astype(jnp.float32).T * blend, axis=0))
    places = jnp.arange(innovation.shape[0], dtype=jnp.int32)
    valid = places % OBS_DEV < obs_count[places // OBS_DEV]
    departures = jnp.where(valid, innovation - equivalent, 0.0)
    return (increment, departures)
```

```python
import math

import jax
import jax.numpy as jnp
from jax import lax
from jax.experimental import pallas as pl
from jax.experimental.pallas import tpu as pltpu
from jax.sharding import PartitionSpec as P

F32, BF16, I32 = jnp.float32, jnp.bfloat16, jnp.int32
MESH = pl.DeviceIdType.MESH
ZH, Y, C = 2, 4, 2
LAT, LON = 4, 8
NX, NY, TX, TY = 128, 1024, 32, 128
TILES = LAT * LON


def iota(shape, dim):
    return lax.broadcasted_iota(I32, shape, dim)


def halves(v):
    high = v.astype(BF16)
    return high, (v - high.astype(F32)).astype(BF16)


def thirds(v):
    high, rest = v.astype(BF16), v - v.astype(BF16).astype(F32)
    return (high, *halves(rest))


def dot(a, b):
    return lax.dot_general(a, b, (((1,), (0,)), ((), ())), preferred_element_type=F32)


def dot_nt(a, b):
    return lax.dot_general(a, b, (((1,), (1,)), ((), ())), preferred_element_type=F32)


def dot_tn(a, b):
    return lax.dot_general(a, b, (((0,), (0,)), ((), ())), preferred_element_type=F32)


def kernel(
    il_b, il_kx, modes, weights, innovation, tgt, col, count, ctrl_hbm, pert_hbm,
    inc_ref, dep_ref,
    ctrl, pert, field, lat_send, lat_recv, lon_send, lon_recv, pk_send, pk_recv,
    total, core_recv, red1, y_recv, red2, z_recv,
    row_send, row_recv, edge_send, edge_recv, val, val_recv, vsum, yc_recv, vsum2, x_recv,
    load_sem, lat_s, lat_r, lon_s, lon_r, pk_s, pk_r, core_s, core_r, y_s, y_r, z_s, z_r,
    row_s, row_r, edge_s, edge_r, val_s, val_r, yc_s, yc_r, x_s, x_r,
):
    mem, a, b = (lax.axis_index(n) for n in ("mem", "lat", "lon"))
    zh, y, c = mem // (Y * C), (mem // C) % Y, mem % C
    q = y * C + c

    def remote(src, dst, s, r, dev):
        return pltpu.make_async_remote_copy(
            src_ref=src, dst_ref=dst, send_sem=s, recv_sem=r, device_id=dev, device_id_type=MESH
        )

    load_c = pltpu.make_async_copy(ctrl_hbm, ctrl, load_sem.at[0])
    load_p = pltpu.make_async_copy(pert_hbm, pert, load_sem.at[1])
    load_c.start()
    load_p.start()
    row_recv[...] = jnp.zeros_like(row_recv)
    edge_recv[...] = jnp.zeros_like(edge_recv)

    barrier = pltpu.get_barrier_semaphore()

    def greet(dev):
        pl.semaphore_signal(barrier, inc=1, device_id=dev, device_id_type=MESH)

    for d in range(1, TILES):
        greet((mem, (a + d // LON) % LAT, (b + d % LON) % LON))
    for d in range(1, Y * C):
        greet((zh * Y * C + (q + d) % (Y * C), a, b))
    for d in range(LON):
        greet(((mem + Y * C) % (ZH * Y * C), a, (b + d) % LON))

    rest_x = (NX - TX * a).astype(F32)
    rest_y = (NY - TY * b).astype(F32)
    load_c.wait()
    for g in range(2):
        il = il_kx[0:1, g * 256 : (g + 1) * 256]
        rows, cols = iota((16, 256), 0), iota((16, 256), 1)
        x = (cols & 31).astype(F32)
        up = jnp.exp((x - 31.0) * il)
        down = jnp.exp(-x * il) - jnp.exp((x - 2.0 * rest_x) * il)
        table = jnp.where(cols >> 5 == (rows & 7), jnp.where(rows < 8, up, down), 0.0)
        high, low = halves(table)
        for m in range(4):
            s = ctrl[m, g * 8 : (g + 1) * 8].reshape(256, 128)
            e = dot(high, s) + dot(low, s)
            lat_send[0, m, g * 8 : (g + 1) * 8, :] = e[0:8]
            lat_send[1, m, g * 8 : (g + 1) * 8, :] = e[8:16]

    pl.semaphore_wait(barrier, TILES - 1 + Y * C - 1 + LON)
    lat_copies = []
    for d in range(1, LAT):
        copy = remote(
            lat_send.at[(a + d) // LAT], lat_recv.at[d - 1], lat_s.at[d - 1], lat_r.at[d - 1],
            (mem, (a + d) % LAT, b),
        )
        copy.start()
        lat_copies.append(copy)

    for g in range(2):
        il = il_kx[0:1, g * 256 : (g + 1) * 256]
        rows, cols = iota((256, 256), 0), iota((256, 256), 1)
        x1, x2 = (rows & 31).astype(F32), (cols & 31).astype(F32)
        near = jnp.exp(-jnp.abs(x1 - x2) * il)
        back = jnp.exp((x1 + x2 - 2.0 * rest_x) * il)
        high, low = halves(jnp.where(rows >> 5 == cols >> 5, near - back, 0.0))
        for m in range(4):
            s = ctrl[m, g * 8 : (g + 1) * 8].reshape(256, 128)
            out = dot(high, s) + dot(low, s)
            field[g * 8 : (g + 1) * 8, m * TX : (m + 1) * TX, :] = out.reshape(8, TX, TY)

    t = tgt[...]
    rel = (((t >> 3) + (LAT - a)) & 3) * LON + (((t & 7) + (LON - b)) & 7)
    marks = jnp.where(iota((TILES, 512), 0) == rel, 1.0, 0.0)
    before = jnp.where(iota((512, 512), 0) < iota((512, 512), 1), 1.0, 0.0).astype(BF16)
    rank = jnp.sum(dot(marks.astype(BF16), before) * marks, axis=0, keepdims=True).astype(I32)
    slot = rel * 32 + rank
    chosen = jnp.where(iota((1024, 512), 0) == slot, 1.0, 0.0).astype(BF16)
    r8 = iota((8, 64), 0)
    level = (r8 >> 2) * 32 + q * 4 + (r8 & 3)
    own = jnp.where(iota((8, 64), 1) == level, 1.0, 0.0).astype(BF16)
    picked = dot_nt(own, weights[...])
    place = col[...]
    r8 = iota((8, 512), 0)
    places = jnp.where(r8 == 0, (place >> 7).astype(F32), (place & 127).astype(F32))
    packed = dot_nt(jnp.concatenate([picked, places], 0).astype(BF16), chosen)
    spot = jnp.broadcast_to(packed[8:9] * 128.0 + packed[9:10], (8, 1024))
    lane = iota((8, 128), 1)
    for k in range(TILES):
        block, j = slice(k // 4 * 128, k // 4 * 128 + 128), k % 4
        w = packed[0:8, block]
        p = spot[:, block]
        w = pltpu.roll(w, (128 - 32 * j) % 128, 1) if j else w
        p = pltpu.roll(p, (160 - 32 * j) % 128, 1) if j != 1 else p
        tile = jnp.where(lane < 32, w, p)
        if k:
            pk_send[k] = tile
        else:
            pk_recv[0] = tile

    ilb = il_b[...]
    carry_l, carry_r = [0.0] * 4, [0.0] * 4
    for d in range(1, LAT):
        lat_copies[d - 1].wait_recv()
        left = jnp.where(a >= d, 1.0, 0.0)
        wl = jnp.exp(-32.0 * (d - 1) * ilb) * left
        wr = jnp.exp(-32.0 * (LAT - 1 - d) * ilb) * (1.0 - left)
        for m in range(4):
            got = lat_recv[d - 1, m]
            carry_l[m] = carry_l[m] + wl * got
            carry_r[m] = carry_r[m] + wr * got
    x = iota((TX, TY), 0).astype(F32)
    ly = iota((8, TY), 1).astype(F32)
    r8 = iota((8, TY), 0)
    for k in range(16):
        il = ilb[k : k + 1]
        ahead = jnp.exp(-(x + 1.0) * il) - jnp.exp((x - 1.0 - 2.0 * rest_x) * il)
        behind = jnp.exp((x - 32.0) * il)
        for m in range(4):
            here = slice(m * TX, (m + 1) * TX)
            field[k, here, :] = (
                field[k, here, :] + ahead * carry_l[m][k : k + 1] + behind * carry_r[m][k : k + 1]
            )
        up = jnp.exp((ly - 127.0) * il)
        down = jnp.exp(-ly * il) - jnp.exp((ly - 2.0 * rest_y) * il)
        th, tl = halves(jnp.where(r8 == 0, up, down))
        fh, fl = halves(field[k])
        e = dot_nt(th, fh) + dot_nt(th, fl) + dot_nt(tl, fh)
        lon_send[0, k : k + 1, :] = e[0:1]
        lon_send[1, k : k + 1, :] = e[1:2]
    lon_copies = []
    for d in range(1, LON):
        copy = remote(
            lon_send.at[(b + d) // LON], lon_recv.at[d - 1], lon_s.at[d - 1], lon_r.at[d - 1],
            (mem, a, (b + d) % LON),
        )
        copy.start()
        lon_copies.append(copy)

    y1, y2 = iota((TY, TY), 0).astype(F32), iota((TY, TY), 1).astype(F32)
    for k in range(16):
        il = ilb[k : k + 1]
        nh, nl = halves(
            jnp.exp(-jnp.abs(y1 - y2) * il) - jnp.exp((y1 + y2 - 2.0 * rest_y) * il)
        )
        fh, fl = halves(field[k])
        field[k] = dot(fh, nh) + dot(fl, nh) + dot(fh, nl)

    spread = jnp.where(iota((512, 64), 0) >> 3 == iota((512, 64), 1), 1.0, 0.0).astype(BF16)
    widen = jnp.where(iota((16, 128), 0) == iota((16, 128), 1) >> 3, 1.0, 0.0).astype(BF16)
    diagonal = (iota((512, 128), 0) & 7) == (iota((512, 128), 1) & 7)
    mh, ml = (
        jnp.where(diagonal, dot(dot(spread, part).astype(BF16), widen), 0.0).astype(BF16)
        for part in halves(modes[...])
    )

    cl, cr = 0.0, 0.0
    for d in range(1, LON):
        lon_copies[d - 1].wait_recv()
        left = jnp.where(b >= d, 1.0, 0.0)
        got = lon_recv[d - 1]
        cl = cl + (jnp.exp(-128.0 * (d - 1) * ilb) * left) * got
        cr = cr + (jnp.exp(-128.0 * (LON - 1 - d) * ilb) * (1.0 - left)) * got
    pk_copies = []
    for k in range(1, TILES):
        copy = remote(
            pk_send.at[k], pk_recv.at[k], pk_s.at[k - 1], pk_r.at[k - 1],
            (mem, (a + k // LON) % LAT, (b + k % LON) % LON),
        )
        copy.start()
        pk_copies.append(copy)
    for k in range(16):
        il = ilb[k : k + 1]
        ahead = jnp.exp(-(ly + 1.0) * il) - jnp.exp((ly - 1.0 - 2.0 * rest_y) * il)
        behind = jnp.exp((ly - 128.0) * il)
        ah, al = halves(jnp.where(r8 == 0, ahead, jnp.where(r8 == 1, behind, 0.0)))
        ch, co = halves(
            jnp.where(r8 == 0, cl[k : k + 1], jnp.where(r8 == 1, cr[k : k + 1], 0.0))
        )
        field[k] = field[k] + (dot_tn(ch, ah) + dot_tn(co, ah) + dot_tn(ch, al))

    load_p.wait()
    for xb in range(4):
        acc = None
        for m in range(4):
            rows = field[:, m * TX + xb * 8 : m * TX + xb * 8 + 8, :].reshape(128, 128)
            fh, fl = halves(rows)
            prof = dot(mh, fh) + dot(mh, fl) + dot(ml, fh)
            p = pert[m, :, xb * 8 : xb * 8 + 8, :].astype(F32).reshape(512, 128)
            acc = prof * p if acc is None else acc + prof * p
        total[:, :, :, xb * 8 : xb * 8 + 8, :] = acc.reshape(8, 2, 4, 8, 128)

    core_copy = remote(
        total.at[:, 1 - c], core_recv, core_s.at[0], core_r.at[0], (mem + 1 - 2 * c, a, b)
    )
    core_copy.start()
    core_copy.wait_recv()
    red1[...] = (total[:, c] + core_recv[...]).reshape(2, 4, 4, TX, TY)
    y_copies = []
    for d in range(1, Y):
        yp = (y + d) % Y
        copy = remote(
            red1.at[:, yp], y_recv.at[d - 1], y_s.at[d - 1], y_r.at[d - 1],
            ((zh * Y + yp) * C + c, a, b),
        )
        copy.start()
        y_copies.append(copy)

    w_all, p_all = jnp.zeros((64, 128), F32), jnp.zeros((64, 128), F32)
    group = iota((64, 128), 1) >> 5
    for da in range(LAT):
        for k in range(max(1, da * LON), (da + 1) * LON):
            pk_copies[k - 1].wait_recv()
        got = pk_recv[da * LON : (da + 1) * LON].reshape(64, 128)
        w = pltpu.roll(got, 32 * da, 1) if da else got
        p = pltpu.roll(got, (32 * da + 96) % 128, 1) if da != 1 else got
        w_all = jnp.where(group == da, w, w_all)
        p_all = jnp.where(group == da, p, p_all)

    for copy in y_copies:
        copy.wait_recv()
    whole = red1[:, y] + y_recv[0] + y_recv[1] + y_recv[2]
    whole = whole.reshape(8, TX, TY)
    red2[...] = whole
    z_copy = remote(
        red2.at[pl.ds((1 - zh) * 4, 4)], z_recv, z_s.at[0], z_r.at[0],
        ((mem + Y * C) % (ZH * Y * C), a, b),
    )

    r8 = iota((8, 128), 0)
    ends = jnp.where(
        (r8 == 0) & (lane == 0) | (r8 == 1) & (lane == 127), 1.0, 0.0
    ).astype(BF16)
    wh, wl = halves(whole.reshape(256, 128))
    row_send[0] = red2[:, TX - 1, :]
    row_send[1] = red2[:, 0, :]
    edge_send[...] = dot_nt(ends, wh) + dot_nt(ends, wl)
    halo = []
    for s in range(2):
        step = 1 - 2 * s
        copy = remote(
            row_send.at[s], row_recv.at[s], row_s.at[s], row_r.at[s],
            (mem, (a + step + LAT) % LAT, b),
        )
        there, back = a + step, a - step
        halo.append((copy, (there >= 0) & (there < LAT), (back >= 0) & (back < LAT)))
    for i, da in enumerate((-1, 0, 1)):
        for j, db in enumerate((-1, 1)):
            copy = remote(
                edge_send, edge_recv.at[i, j], edge_s.at[i, j], edge_r.at[i, j],
                (mem, (a - da + LAT) % LAT, (b - db + LON) % LON),
            )
            at, bt, af, bf = a - da, b - db, a + da, b + db
            halo.append((
                copy,
                (at >= 0) & (at < LAT) & (bt >= 0) & (bt < LON),
                (af >= 0) & (af < LAT) & (bf >= 0) & (bf < LON),
            ))
    for copy, sends, _ in halo:
        pl.when(sends)(copy.start)
    z_copy.start()
    for copy, _, gets in halo:
        pl.when(gets)(copy.wait_recv)

    top, bottom = halves(row_recv[0]), halves(row_recv[1])
    r8w = iota((8, 256), 0)
    l8w = iota((8, 256), 1)

    def sides(i):
        both = jnp.where(
            r8w % 2 == 0, edge_recv[i, 0][1:2], edge_recv[i, 1][0:1]
        )
        high = both.astype(BF16).astype(F32)
        return jnp.where(r8w < 2, high, jnp.where(r8w < 4, both - high, 0.0)).astype(BF16)

    around = sides(1)
    above = dot_nt(jnp.where(l8w == r8w * 32 + 31, 1.0, 0.0).astype(BF16), sides(0))
    below = dot_nt(jnp.where(l8w == r8w * 32, 1.0, 0.0).astype(BF16), sides(2))
    above, below = above.astype(BF16), below.astype(BF16)
    ys, xs = iota((TY, 128), 0), iota((TX, 128), 0)

    def blend(near, far, at):
        return jnp.where(at == near, 0.75, 0.0) + jnp.where(at == far, 0.25, 0.0)

    val_copies = []
    for db in range(LON):
        spot = p_all[db * 8 : db * 8 + 1].astype(I32)
        i, j = spot >> 8, spot & 255
        nx, ny = i >> 1, j >> 1
        fx, fy = nx + 2 * (i & 1) - 1, ny + 2 * (j & 1) - 1
        cols = blend(ny, fy, ys).astype(BF16)
        side = jnp.where(
            r8 < 4, jnp.where(r8 % 2 == 0, blend(ny, fy, -1), blend(ny, fy, TY)), 0.0
        ).astype(BF16)
        inner = dot(wh, cols) + dot(wl, cols) + dot_tn(around, side)
        inner = jnp.sum(inner.reshape(8, TX, 128) * blend(nx, fx, xs)[None], axis=1)
        up = dot(top[0], cols) + dot(top[1], cols) + dot(above, side)
        down = dot(bottom[0], cols) + dot(bottom[1], cols) + dot(below, side)
        inner = inner + up * blend(nx, fx, -1) + down * blend(nx, fx, TX)
        val[db] = jnp.sum(inner * w_all[db * 8 : db * 8 + 8], axis=0, keepdims=True)
        for zo in range(ZH):
            n = zo * LON + db
            if n:
                copy = remote(
                    val.at[db], val_recv.at[n], val_s.at[n - 1], val_r.at[n - 1],
                    ((mem + zo * Y * C) % (ZH * Y * C), a, (b - db + LON) % LON),
                )
                copy.start()
                val_copies.append(copy)
    val_recv[0] = val[0]
    for copy in val_copies:
        copy.wait_recv()
    for db in range(LON):
        vsum[db : db + 1, :] = val_recv[db] + val_recv[LON + db]
    yc_copies = []
    for d in range(1, Y * C):
        copy = remote(
            vsum, yc_recv.at[d - 1], yc_s.at[d - 1], yc_r.at[d - 1],
            (zh * Y * C + (q + d) % (Y * C), a, b),
        )
        copy.start()
        yc_copies.append(copy)
    for copy in yc_copies:
        copy.wait_recv()
    mine = vsum[...]
    for d in range(Y * C - 1):
        mine = mine + yc_recv[d]
    vsum2[...] = mine
    x_copies = []
    for d in range(1, LAT):
        copy = remote(
            vsum2, x_recv.at[d - 1], x_s.at[d - 1], x_r.at[d - 1], (mem, (a + d) % LAT, b)
        )
        copy.start()
        x_copies.append(copy)
    for copy in x_copies:
        copy.wait_recv()
    table = jnp.concatenate([mine, x_recv[2], x_recv[1], x_recv[0]], 0)
    marks = marks.astype(BF16)
    found = sum(dot_tn(part, marks) for part in thirds(table))
    here = iota((128, 512), 0) == (rel >> 3) * 32 + rank
    equivalent = jnp.sum(jnp.where(here, found, 0.0), axis=0, keepdims=True)
    live = iota((1, 512), 1) < count[0]
    dep_ref[...] = jnp.where(live, innovation[...] - equivalent, 0.0)

    z_copy.wait_recv()
    inc_ref[...] = red2[pl.ds(zh * 4, 4)] + z_recv[...]
    for copy in (*lat_copies, *lon_copies, *pk_copies, core_copy, *y_copies, z_copy):
        copy.wait_send()
    for copy in (*val_copies, *yc_copies, *x_copies):
        copy.wait_send()
    for copy, sends, _ in halo:
        pl.when(sends)(copy.wait_send)


def per_device(
    perturbation, control, filter_length, modes, obs_weights, innovation, obs_tile,
    obs_column, obs_count,
):
    il = 1.0 / filter_length
    rate = jnp.exp(-il)
    gain = (1.0 - rate) / ((1.0 + rate) * math.sqrt(4 * ZH * Y * C - 1))
    vmem = pl.BlockSpec(memory_space=pltpu.VMEM)
    anywhere = pl.BlockSpec(memory_space=pl.ANY)
    smem = pl.BlockSpec(memory_space=pltpu.SMEM)
    f32 = lambda *shape: pltpu.VMEM(shape, F32)
    sem = lambda *shape: pltpu.SemaphoreType.DMA(shape)
    pairs = lambda *shape: [sem(*shape), sem(*shape)]
    increment, departures = pl.pallas_call(
        kernel,
        out_shape=(
            jax.ShapeDtypeStruct((4, TX, TY), F32),
            jax.ShapeDtypeStruct((1, 512), F32),
        ),
        in_specs=[vmem] * 7 + [smem] + [anywhere] * 2,
        out_specs=(vmem, vmem),
        scratch_shapes=[
            pltpu.VMEM((4, 16, TX, TY), BF16), pltpu.VMEM((4, 64, TX, TY), BF16),
            f32(16, 128, TY),
            f32(2, 4, 16, TY), f32(LAT - 1, 4, 16, TY),
            f32(2, 16, 128), f32(LON - 1, 16, 128),
            f32(TILES, 8, 128), f32(TILES, 8, 128),
            f32(8, 2, 4, TX, TY), f32(8, 4, TX, TY),
            f32(2, 4, 4, TX, TY), f32(Y - 1, 2, 4, TX, TY),
            f32(8, TX, TY), f32(4, TX, TY),
            f32(2, 8, 128), f32(2, 8, 128), f32(8, 256), f32(3, 2, 8, 256),
            f32(LON, 1, 128), f32(ZH * LON, 1, 128), f32(8, 128),
            f32(Y * C - 1, 8, 128), f32(8, 128), f32(LAT - 1, 8, 128),
            sem(2), *pairs(LAT - 1), *pairs(LON - 1), *pairs(TILES - 1), *pairs(1),
            *pairs(Y - 1), *pairs(1), *pairs(2), *pairs(3, 2), *pairs(ZH * LON - 1),
            *pairs(Y * C - 1), *pairs(LAT - 1),
        ],
        compiler_params=pltpu.CompilerParams(
            collective_id=0, has_side_effects=True, vmem_limit_bytes=48 * 2**20
        ),
        name="hybrid",
    )(
        jnp.broadcast_to(il[:, None], (16, 128)),
        jnp.broadcast_to(jnp.repeat(il, TX)[None], (8, 512)),
        modes * gain[None, :],
        obs_weights,
        innovation.reshape(1, 512),
        obs_tile.reshape(1, 512),
        obs_column.reshape(1, 512),
        obs_count,
        control,
        perturbation,
    )
    return increment, departures.reshape(512)


def solution(mesh):
    placed = (
        P("mem", None, "lat", "lon"),
        P("mem", None, "lat", "lon"),
        P(),
        P(),
        P(("lat", "lon"), None),
        P(("lat", "lon")),
        P(("lat", "lon"), None),
        P(("lat", "lon")),
        P(("lat", "lon")),
    )
    return jax.shard_map(
        per_device,
        mesh=mesh,
        in_specs=placed,
        out_specs=(P("mem", "lat", "lon"), P(("lat", "lon"))),
        check_vma=False,
    )
```

```python
import math

import jax
import jax.numpy as jnp
from jax import lax
from jax.experimental import pallas as pl
from jax.experimental.pallas import tpu as pltpu
from jax.sharding import PartitionSpec as P

F32, BF16, I32 = jnp.float32, jnp.bfloat16, jnp.int32
MESH = pl.DeviceIdType.MESH
ZH, Y, C = 2, 4, 2
LAT, LON = 4, 8
NX, NY, TX, TY = 128, 1024, 32, 128
TILES = LAT * LON


def iota(shape, dim):
    return lax.broadcasted_iota(I32, shape, dim)


def halves(v):
    high = v.astype(BF16)
    return high, (v - high.astype(F32)).astype(BF16)


def thirds(v):
    high, rest = v.astype(BF16), v - v.astype(BF16).astype(F32)
    return (high, *halves(rest))


def dot(a, b):
    return lax.dot_general(a, b, (((1,), (0,)), ((), ())), preferred_element_type=F32)


def dot_nt(a, b):
    return lax.dot_general(a, b, (((1,), (1,)), ((), ())), preferred_element_type=F32)


def dot_tn(a, b):
    return lax.dot_general(a, b, (((0,), (0,)), ((), ())), preferred_element_type=F32)


def kernel(
    length_hbm, modes_hbm, weights_hbm, innovation_hbm, tgt_hbm, col_hbm, count, ctrl_hbm, pert_hbm,
    inc_ref, dep_ref,
    length, modes, weights, innovation, tgt, col,
    ctrl, pert, field, lat_send, lat_recv, lon_send, lon_recv, pk_send, pk_recv,
    total, core_recv, red1, y_recv, red2, z_recv,
    row_send, row_recv, edge_send, edge_recv, val, val_recv, vsum, yc_recv, vsum2, x_recv,
    load_sem, lat_s, lat_r, lon_s, lon_r, pk_s, pk_r, core_s, core_r, y_s, y_r, z_s, z_r,
    row_s, row_r, edge_s, edge_r, val_s, val_r, yc_s, yc_r, x_s, x_r,
):
    mem, a, b = (lax.axis_index(n) for n in ("mem", "lat", "lon"))
    zh, y, c = mem // (Y * C), (mem // C) % Y, mem % C
    q = y * C + c

    def remote(src, dst, s, r, dev):
        return pltpu.make_async_remote_copy(
            src_ref=src, dst_ref=dst, send_sem=s, recv_sem=r, device_id=dev, device_id_type=MESH
        )

    loads = [
        pltpu.make_async_copy(src, dst, load_sem.at[n])
        for n, (src, dst) in enumerate((
            (length_hbm, length), (ctrl_hbm, ctrl), (tgt_hbm, tgt), (col_hbm, col),
            (weights_hbm, weights), (modes_hbm, modes), (innovation_hbm, innovation),
            (pert_hbm, pert),
        ))
    ]
    for load in loads:
        load.start()
    row_recv[...] = jnp.zeros_like(row_recv)
    edge_recv[...] = jnp.zeros_like(edge_recv)

    barrier = pltpu.get_barrier_semaphore()

    def greet(dev):
        pl.semaphore_signal(barrier, inc=1, device_id=dev, device_id_type=MESH)

    for d in range(1, TILES):
        greet((mem, (a + d // LON) % LAT, (b + d % LON) % LON))
    for d in range(1, Y * C):
        greet((zh * Y * C + (q + d) % (Y * C), a, b))
    for d in range(LON):
        greet(((mem + Y * C) % (ZH * Y * C), a, (b + d) % LON))

    rest_x = (NX - TX * a).astype(F32)
    rest_y = (NY - TY * b).astype(F32)
    loads[0].wait()
    ilc = jnp.where(iota((16, 16), 0) == iota((16, 16), 1), 1.0 / length[...], 0.0)
    ilc = jnp.sum(ilc, axis=1, keepdims=True)
    ilb = jnp.broadcast_to(ilc, (16, 128))
    il_kx = jnp.where(iota((16, 512), 0) == iota((16, 512), 1) >> 5, ilc, 0.0)
    il_kx = jnp.sum(il_kx, axis=0, keepdims=True)
    loads[1].wait()
    for g in range(2):
        il = il_kx[0:1, g * 256 : (g + 1) * 256]
        rows, cols = iota((16, 256), 0), iota((16, 256), 1)
        x = (cols & 31).astype(F32)
        up = jnp.exp((x - 31.0) * il)
        down = jnp.exp(-x * il) - jnp.exp((x - 2.0 * rest_x) * il)
        table = jnp.where(cols >> 5 == (rows & 7), jnp.where(rows < 8, up, down), 0.0)
        high, low = halves(table)
        for m in range(4):
            s = ctrl[m, g * 8 : (g + 1) * 8].reshape(256, 128)
            e = dot(high, s) + dot(low, s)
            lat_send[0, m, g * 8 : (g + 1) * 8, :] = e[0:8]
            lat_send[1, m, g * 8 : (g + 1) * 8, :] = e[8:16]

    pl.semaphore_wait(barrier, TILES - 1 + Y * C - 1 + LON)
    lat_copies = []
    for d in range(1, LAT):
        copy = remote(
            lat_send.at[(a + d) // LAT], lat_recv.at[d - 1], lat_s.at[d - 1], lat_r.at[d - 1],
            (mem, (a + d) % LAT, b),
        )
        copy.start()
        lat_copies.append(copy)

    for g in range(2):
        il = il_kx[0:1, g * 256 : (g + 1) * 256]
        rows, cols = iota((256, 256), 0), iota((256, 256), 1)
        x1, x2 = (rows & 31).astype(F32), (cols & 31).astype(F32)
        near = jnp.exp(-jnp.abs(x1 - x2) * il)
        back = jnp.exp((x1 + x2 - 2.0 * rest_x) * il)
        high, low = halves(jnp.where(rows >> 5 == cols >> 5, near - back, 0.0))
        for m in range(4):
            s = ctrl[m, g * 8 : (g + 1) * 8].reshape(256, 128)
            out = dot(high, s) + dot(low, s)
            field[g * 8 : (g + 1) * 8, m * TX : (m + 1) * TX, :] = out.reshape(8, TX, TY)

    for load in loads[2:5]:
        load.wait()
    t = tgt[...]
    rel = (((t >> 3) + (LAT - a)) & 3) * LON + (((t & 7) + (LON - b)) & 7)
    marks = jnp.where(iota((TILES, 512), 0) == rel, 1.0, 0.0)
    before = jnp.where(iota((512, 512), 0) < iota((512, 512), 1), 1.0, 0.0).astype(BF16)
    rank = jnp.sum(dot(marks.astype(BF16), before) * marks, axis=0, keepdims=True).astype(I32)
    slot = rel * 32 + rank
    chosen = jnp.where(iota((1024, 512), 0) == slot, 1.0, 0.0).astype(BF16)
    r32 = iota((32, 64), 0)
    level = (r32 >> 2) * 8 + c * 4 + (r32 & 3)
    own = jnp.where(iota((32, 64), 1) == level, 1.0, 0.0).astype(BF16)
    picked = dot(own, weights[...])
    place = col[...]
    r8 = iota((8, 512), 0)
    places = jnp.where(r8 == 0, (place >> 7).astype(F32), (place & 127).astype(F32))
    packed = dot_nt(jnp.concatenate([picked, places], 0).astype(BF16), chosen)
    spot = jnp.broadcast_to(packed[32:33] * 128.0 + packed[33:34], (8, 1024))
    group = iota((8, 128), 1) >> 5

    def turned(v, quarters):
        return pltpu.roll(v, 32 * (quarters % 4), 1) if quarters % 4 else v

    for k in range(TILES):
        block, j = slice(k // 4 * 128, k // 4 * 128 + 128), k % 4
        tile = turned(packed[0:8, block], -j)
        for g in range(1, 4):
            tile = jnp.where(group == g, turned(packed[8 * g : 8 * g + 8, block], g - j), tile)
        into = pk_send if k else pk_recv
        into[k, 0:8, :] = tile
        into[k, 8:9, :] = turned(spot[:, block], -j)[0:1]

    carry_l, carry_r = [0.0] * 4, [0.0] * 4
    for d in range(1, LAT):
        lat_copies[d - 1].wait_recv()
        left = jnp.where(a >= d, 1.0, 0.0)
        wl = jnp.exp(-32.0 * (d - 1) * ilb) * left
        wr = jnp.exp(-32.0 * (LAT - 1 - d) * ilb) * (1.0 - left)
        for m in range(4):
            got = lat_recv[d - 1, m]
            carry_l[m] = carry_l[m] + wl * got
            carry_r[m] = carry_r[m] + wr * got
    x = iota((TX, TY), 0).astype(F32)
    ly = iota((8, TY), 1).astype(F32)
    r8 = iota((8, TY), 0)
    for k in range(16):
        il = ilb[k : k + 1]
        ahead = jnp.exp(-(x + 1.0) * il) - jnp.exp((x - 1.0 - 2.0 * rest_x) * il)
        behind = jnp.exp((x - 32.0) * il)
        for m in range(4):
            here = slice(m * TX, (m + 1) * TX)
            field[k, here, :] = (
                field[k, here, :] + ahead * carry_l[m][k : k + 1] + behind * carry_r[m][k : k + 1]
            )
        up = jnp.exp((ly - 127.0) * il)
        down = jnp.exp(-ly * il) - jnp.exp((ly - 2.0 * rest_y) * il)
        th, tl = halves(jnp.where(r8 == 0, up, down))
        fh, fl = halves(field[k])
        e = dot_nt(th, fh) + dot_nt(th, fl) + dot_nt(tl, fh)
        lon_send[0, k : k + 1, :] = e[0:1]
        lon_send[1, k : k + 1, :] = e[1:2]
    lon_copies = []
    for d in range(1, LON):
        copy = remote(
            lon_send.at[(b + d) // LON], lon_recv.at[d - 1], lon_s.at[d - 1], lon_r.at[d - 1],
            (mem, a, (b + d) % LON),
        )
        copy.start()
        lon_copies.append(copy)

    pk_copies = []
    for k in range(1, TILES):
        copy = remote(
            pk_send.at[k], pk_recv.at[k], pk_s.at[k - 1], pk_r.at[k - 1],
            (mem, (a + k // LON) % LAT, (b + k % LON) % LON),
        )
        copy.start()
        pk_copies.append(copy)

    y1, y2 = iota((TY, TY), 0).astype(F32), iota((TY, TY), 1).astype(F32)
    for k in range(16):
        il = ilb[k : k + 1]
        nh, nl = halves(
            jnp.exp(-jnp.abs(y1 - y2) * il) - jnp.exp((y1 + y2 - 2.0 * rest_y) * il)
        )
        fh, fl = halves(field[k])
        field[k] = dot(fh, nh) + dot(fl, nh) + dot(fh, nl)

    loads[5].wait()
    half = 0.5 * ilc
    sq = half * half
    gain = half * (1.0 - sq * (1.0 / 3.0 - sq * (2.0 / 15.0 - sq * (17.0 / 315.0))))
    scaled = modes[...] * (gain * (1.0 / math.sqrt(4 * ZH * Y * C - 1)))
    spread = jnp.where(iota((512, 64), 0) >> 3 == iota((512, 64), 1), 1.0, 0.0).astype(BF16)
    widen = jnp.where(iota((16, 128), 0) == iota((16, 128), 1) >> 3, 1.0, 0.0).astype(BF16)
    diagonal = (iota((512, 128), 0) & 7) == (iota((512, 128), 1) & 7)
    mh, ml = (
        jnp.where(diagonal, dot(spread, dot_tn(part, widen).astype(BF16)), 0.0).astype(BF16)
        for part in halves(scaled)
    )

    cl, cr = 0.0, 0.0
    for d in range(1, LON):
        lon_copies[d - 1].wait_recv()
        left = jnp.where(b >= d, 1.0, 0.0)
        got = lon_recv[d - 1]
        cl = cl + (jnp.exp(-128.0 * (d - 1) * ilb) * left) * got
        cr = cr + (jnp.exp(-128.0 * (LON - 1 - d) * ilb) * (1.0 - left)) * got
    for k in range(16):
        il = ilb[k : k + 1]
        ahead = jnp.exp(-(ly + 1.0) * il) - jnp.exp((ly - 1.0 - 2.0 * rest_y) * il)
        behind = jnp.exp((ly - 128.0) * il)
        ah, al = halves(jnp.where(r8 == 0, ahead, jnp.where(r8 == 1, behind, 0.0)))
        ch, co = halves(
            jnp.where(r8 == 0, cl[k : k + 1], jnp.where(r8 == 1, cr[k : k + 1], 0.0))
        )
        field[k] = field[k] + (dot_tn(ch, ah) + dot_tn(co, ah) + dot_tn(ch, al))

    loads[7].wait()
    core_copies = []
    for xb in range(4):
        acc = None
        for m in range(4):
            rows = field[:, m * TX + xb * 8 : m * TX + xb * 8 + 8, :].reshape(128, 128)
            fh, fl = halves(rows)
            prof = dot(mh, fh) + dot(mh, fl) + dot(ml, fh)
            p = pert[m, :, xb * 8 : xb * 8 + 8, :].astype(F32).reshape(512, 128)
            acc = prof * p if acc is None else acc + prof * p
        total[:, :, :, xb * 8 : xb * 8 + 8, :] = acc.reshape(8, 2, 4, 8, 128)
        part = pl.ds(xb * 8, 8)
        copy = remote(
            total.at[:, 1 - c, :, part, :], core_recv.at[:, :, part, :],
            core_s.at[xb], core_r.at[xb], (mem + 1 - 2 * c, a, b),
        )
        copy.start()
        core_copies.append(copy)

    for copy in core_copies:
        copy.wait_recv()
    whole = total[:, c] + core_recv[...]
    red1[...] = whole.reshape(2, 4, 4, TX, TY)
    y_copies = []
    for d in range(1, Y):
        yp = (y + d) % Y
        copy = remote(
            red1.at[:, yp], y_recv.at[d - 1], y_s.at[d - 1], y_r.at[d - 1],
            ((zh * Y + yp) * C + c, a, b),
        )
        copy.start()
        y_copies.append(copy)

    lane = iota((8, 128), 1)
    r8 = iota((8, 128), 0)
    ends = jnp.where(
        (r8 == 0) & (lane == 0) | (r8 == 1) & (lane == 127), 1.0, 0.0
    ).astype(BF16)
    wh, wl = halves(whole.reshape(1024, 128))
    row_send[0] = red1[:, :, :, TX - 1, :].reshape(32, 128)
    row_send[1] = red1[:, :, :, 0, :].reshape(32, 128)
    edge_send[...] = (dot_nt(ends, wh) + dot_nt(ends, wl))[0:2]
    halo = []
    for s in range(2):
        step = 1 - 2 * s
        copy = remote(
            row_send.at[s], row_recv.at[s], row_s.at[s], row_r.at[s],
            (mem, (a + step + LAT) % LAT, b),
        )
        there, back = a + step, a - step
        halo.append((copy, (there >= 0) & (there < LAT), (back >= 0) & (back < LAT)))
    for i, da in enumerate((-1, 0, 1)):
        for j, db in enumerate((-1, 1)):
            copy = remote(
                edge_send, edge_recv.at[i, j], edge_s.at[i, j], edge_r.at[i, j],
                (mem, (a - da + LAT) % LAT, (b - db + LON) % LON),
            )
            at, bt, af, bf = a - da, b - db, a + da, b + db
            halo.append((
                copy,
                (at >= 0) & (at < LAT) & (bt >= 0) & (bt < LON),
                (af >= 0) & (af < LAT) & (bf >= 0) & (bf < LON),
            ))
    for copy, sends, _ in halo:
        pl.when(sends)(copy.start)

    w_all, p_all = [jnp.zeros((64, 128), F32)] * 4, jnp.zeros((8, 128), F32)
    g64 = iota((64, 128), 1) >> 5
    for da in range(LAT):
        for k in range(max(1, da * LON), (da + 1) * LON):
            pk_copies[k - 1].wait_recv()
        got = pk_recv[da * LON : (da + 1) * LON, 0:8, :].reshape(64, 128)
        w_all = [
            jnp.where(g64 == da, turned(got, da - g), w) for g, w in enumerate(w_all)
        ]
        p_all = jnp.where(
            group == da, turned(pk_recv[da * LON : (da + 1) * LON, 8, :], da), p_all
        )
    ys, xs = iota((TY, 128), 0), iota((TX, 128), 0)

    def blend(near, far, at):
        return jnp.where(at == near, 0.75, 0.0) + jnp.where(at == far, 0.25, 0.0)

    double = jnp.concatenate([wh, wl], 1)
    spots = []
    for db in range(LON):
        spot = p_all[db : db + 1].astype(I32)
        i, j = spot >> 8, spot & 255
        nx, ny = i >> 1, j >> 1
        fx, fy = nx + 2 * (i & 1) - 1, ny + 2 * (j & 1) - 1
        cols, rows = blend(ny, fy, ys).astype(BF16), blend(nx, fx, xs)
        inner = dot(double, jnp.concatenate([cols, cols], 0))
        inner = jnp.sum(inner.reshape(32, TX, 128) * rows[None], axis=1)
        around = [blend(ny, fy, -1), blend(ny, fy, TY), blend(nx, fx, -1), blend(nx, fx, TX)]
        spots.append((inner, cols, rows.astype(BF16), *around))

    for copy, _, gets in halo:
        pl.when(gets)(copy.wait_recv)
    beyond = jnp.concatenate([*halves(row_recv[0]), *halves(row_recv[1])], 0)
    z32, l32 = iota((32, 1024), 0), iota((32, 1024), 1)
    fold = jnp.where(iota((1024, TX), 0) & 31 == iota((1024, TX), 1), 1.0, 0.0).astype(BF16)

    def at_level(line, where):
        return jnp.where(where, line, 0.0)

    left, right = edge_recv[1, 0][1:2], edge_recv[1, 1][0:1]
    same = l32 >> 5 == z32
    beside = jnp.concatenate(
        [*halves(at_level(left, same)), *halves(at_level(right, same))], 0
    )
    beside = dot(beside, fold).astype(BF16)
    corner = [
        jnp.sum(at_level(edge_recv[i, j][1 - j : 2 - j], l32 == z32 * 32 + x), 1, keepdims=True)
        for i, x in ((0, TX - 1), (2, 0))
        for j in range(2)
    ]
    val_copies = []
    for db in range(LON):
        inner, cols, rows, west, east, north, south = spots[db]
        ud = dot(beyond, cols)
        lr = dot(beside, rows)
        up = ud[0:32] + ud[32:64] + corner[0] * west + corner[1] * east
        down = ud[64:96] + ud[96:128] + corner[2] * west + corner[3] * east
        inner = inner + (lr[0:32] + lr[32:64]) * west + (lr[64:96] + lr[96:128]) * east
        inner = inner + up * north + down * south
        w = jnp.concatenate([w[db * 8 : db * 8 + 8] for w in w_all], 0)
        val[db] = jnp.sum(inner * w, axis=0, keepdims=True)
        for zo in range(ZH):
            n = zo * LON + db
            if n:
                copy = remote(
                    val.at[db], val_recv.at[n], val_s.at[n - 1], val_r.at[n - 1],
                    ((mem + zo * Y * C) % (ZH * Y * C), a, (b - db + LON) % LON),
                )
                copy.start()
                val_copies.append(copy)

    for copy in y_copies:
        copy.wait_recv()
    red2[...] = red1[:, y] + y_recv[0] + y_recv[1] + y_recv[2]
    z_copy = remote(
        red2.at[1 - zh], z_recv, z_s.at[0], z_r.at[0],
        ((mem + Y * C) % (ZH * Y * C), a, b),
    )
    z_copy.start()

    val_recv[0] = val[0]
    for copy in val_copies:
        copy.wait_recv()
    for db in range(LON):
        vsum[db : db + 1, :] = val_recv[db] + val_recv[LON + db]
    yc_copies = []
    for d in range(1, Y * C):
        copy = remote(
            vsum, yc_recv.at[d - 1], yc_s.at[d - 1], yc_r.at[d - 1],
            (zh * Y * C + (q + d) % (Y * C), a, b),
        )
        copy.start()
        yc_copies.append(copy)
    for copy in yc_copies:
        copy.wait_recv()
    mine = vsum[...]
    for d in range(Y * C - 1):
        mine = mine + yc_recv[d]
    vsum2[...] = mine
    x_copies = []
    for d in range(1, LAT):
        copy = remote(
            vsum2, x_recv.at[d - 1], x_s.at[d - 1], x_r.at[d - 1], (mem, (a + d) % LAT, b)
        )
        copy.start()
        x_copies.append(copy)
    for copy in x_copies:
        copy.wait_recv()
    table = jnp.concatenate([mine, x_recv[2], x_recv[1], x_recv[0]], 0)
    marks = marks.astype(BF16)
    found = sum(dot_tn(part, marks) for part in thirds(table))
    here = iota((128, 512), 0) == (rel >> 3) * 32 + rank
    equivalent = jnp.sum(jnp.where(here, found, 0.0), axis=0, keepdims=True)
    loads[6].wait()
    live = iota((1, 512), 1) < count[0]
    dep_ref[...] = jnp.where(live, innovation[...] - equivalent, 0.0)

    z_copy.wait_recv()
    inc_ref[...] = red2[zh] + z_recv[...]
    for copy in (*lat_copies, *lon_copies, *pk_copies, *core_copies, *y_copies, z_copy):
        copy.wait_send()
    for copy in (*val_copies, *yc_copies, *x_copies):
        copy.wait_send()
    for copy, sends, _ in halo:
        pl.when(sends)(copy.wait_send)


def per_device(
    perturbation, control, filter_length, modes, obs_weights, innovation, obs_tile,
    obs_column, obs_count,
):
    vmem = pl.BlockSpec(memory_space=pltpu.VMEM)
    hbm = pl.BlockSpec(memory_space=pltpu.HBM)
    smem = pl.BlockSpec(memory_space=pltpu.SMEM)
    f32 = lambda *shape: pltpu.VMEM(shape, F32)
    sem = lambda *shape: pltpu.SemaphoreType.DMA(shape)
    pairs = lambda *shape: [sem(*shape), sem(*shape)]
    increment, departures = pl.pallas_call(
        kernel,
        out_shape=(
            jax.ShapeDtypeStruct((4, TX, TY), F32),
            jax.ShapeDtypeStruct((1, 512), F32),
        ),
        in_specs=[hbm] * 6 + [smem] + [hbm] * 2,
        out_specs=(vmem, vmem),
        scratch_shapes=[
            f32(1, 16), f32(16, 64), pltpu.VMEM((64, 512), BF16), f32(1, 512),
            pltpu.VMEM((1, 512), I32), pltpu.VMEM((1, 512), I32),
            pltpu.VMEM((4, 16, TX, TY), BF16), pltpu.VMEM((4, 64, TX, TY), BF16),
            f32(16, 128, TY),
            f32(2, 4, 16, TY), f32(LAT - 1, 4, 16, TY),
            f32(2, 16, 128), f32(LON - 1, 16, 128),
            f32(TILES, 9, 128), f32(TILES, 9, 128),
            f32(8, 2, 4, TX, TY), f32(8, 4, TX, TY),
            f32(2, 4, 4, TX, TY), f32(Y - 1, 2, 4, TX, TY),
            f32(2, 4, TX, TY), f32(4, TX, TY),
            f32(2, 32, 128), f32(2, 32, 128), f32(2, 1024), f32(3, 2, 2, 1024),
            f32(LON, 1, 128), f32(ZH * LON, 1, 128), f32(8, 128),
            f32(Y * C - 1, 8, 128), f32(8, 128), f32(LAT - 1, 8, 128),
            sem(8), *pairs(LAT - 1), *pairs(LON - 1), *pairs(TILES - 1), *pairs(4),
            *pairs(Y - 1), *pairs(1), *pairs(2), *pairs(3, 2), *pairs(ZH * LON - 1),
            *pairs(Y * C - 1), *pairs(LAT - 1),
        ],
        compiler_params=pltpu.CompilerParams(
            collective_id=0, has_side_effects=True, vmem_limit_bytes=60_000_000
        ),
        name="hybrid",
    )(
        filter_length.reshape(1, 16),
        modes.T,
        obs_weights.T,
        innovation.reshape(1, 512),
        obs_tile.reshape(1, 512),
        obs_column.reshape(1, 512),
        obs_count,
        control,
        perturbation,
    )
    return increment, departures.reshape(512)


def solution(mesh):
    placed = (
        P("mem", None, "lat", "lon"),
        P("mem", None, "lat", "lon"),
        P(),
        P(),
        P(("lat", "lon"), None),
        P(("lat", "lon")),
        P(("lat", "lon"), None),
        P(("lat", "lon")),
        P(("lat", "lon")),
    )
    return jax.shard_map(
        per_device,
        mesh=mesh,
        in_specs=placed,
        out_specs=(P("mem", "lat", "lon"), P(("lat", "lon"))),
        check_vma=False,
    )
```

```python
import math

import jax
import jax.numpy as jnp
from jax import lax
from jax.experimental import pallas as pl
from jax.experimental.pallas import tpu as pltpu
from jax.sharding import PartitionSpec as P

F32, BF16, I32 = jnp.float32, jnp.bfloat16, jnp.int32
MESH = pl.DeviceIdType.MESH
ZH, Y, C = 2, 4, 2
LAT, LON = 4, 8
NX, NY, TX, TY = 128, 1024, 32, 128
TILES = LAT * LON


def iota(shape, dim):
    return lax.broadcasted_iota(I32, shape, dim)


def halves(v):
    high = v.astype(BF16)
    return high, (v - high.astype(F32)).astype(BF16)


def thirds(v):
    high, rest = v.astype(BF16), v - v.astype(BF16).astype(F32)
    return (high, *halves(rest))


def dot(a, b):
    return lax.dot_general(a, b, (((1,), (0,)), ((), ())), preferred_element_type=F32)


def dot_nt(a, b):
    return lax.dot_general(a, b, (((1,), (1,)), ((), ())), preferred_element_type=F32)


def dot_tn(a, b):
    return lax.dot_general(a, b, (((0,), (0,)), ((), ())), preferred_element_type=F32)


def kernel(
    length_hbm, modes_hbm, weights_hbm, innovation_hbm, tgt_hbm, col_hbm, count, ctrl_hbm, pert_hbm,
    inc_hbm, dep_hbm,
    length, modes, weights, innovation, tgt, col,
    ctrl, pert, field, lat_send, lat_recv, lon_send, lon_recv, pk_send, pk_recv,
    total, core_recv, red1, y_recv, red2, z_recv,
    row_send, row_recv, edge_send, edge_recv, val, val_recv, vsum, last_send, last_recv, inc_ref, dep_ref,
    load_sem, lat_s, lat_r, lon_s, lon_r, pk_s, pk_r, core_s, core_r, y_s, y_r, z_s, z_r,
    row_s, row_r, edge_s, edge_r, val_s, val_r, last_s, last_r,
):
    mem, a, b = (lax.axis_index(n) for n in ("mem", "lat", "lon"))
    zh, y, c = mem // (Y * C), (mem // C) % Y, mem % C
    q = y * C + c

    def remote(src, dst, s, r, dev):
        return pltpu.make_async_remote_copy(
            src_ref=src, dst_ref=dst, send_sem=s, recv_sem=r, device_id=dev, device_id_type=MESH
        )

    loads = [
        pltpu.make_async_copy(src, dst, load_sem.at[n])
        for n, (src, dst) in enumerate((
            (length_hbm, length), (ctrl_hbm, ctrl), (tgt_hbm, tgt), (col_hbm, col),
            (weights_hbm, weights), (modes_hbm, modes), (innovation_hbm, innovation),
            (pert_hbm, pert),
        ))
    ]
    for load in loads:
        load.start()
    row_recv[...] = jnp.zeros_like(row_recv)
    edge_recv[...] = jnp.zeros_like(edge_recv)

    barrier = pltpu.get_barrier_semaphore()

    def greet(dev):
        pl.semaphore_signal(barrier, inc=1, device_id=dev, device_id_type=MESH)

    for d in range(1, TILES):
        greet((mem, (a + d // LON) % LAT, (b + d % LON) % LON))
    for d in range(1, Y * C):
        greet((zh * Y * C + (q + d) % (Y * C), a, b))
    for d in range(LON):
        greet(((mem + Y * C) % (ZH * Y * C), a, (b + d) % LON))
    for da in range(1, LAT):
        for d in range(1, Y * C):
            greet((zh * Y * C + (q + d) % (Y * C), (a + da) % LAT, b))

    rest_x = (NX - TX * a).astype(F32)
    rest_y = (NY - TY * b).astype(F32)
    loads[0].wait()
    ilc = jnp.where(iota((16, 16), 0) == iota((16, 16), 1), 1.0 / length[...], 0.0)
    ilc = jnp.sum(ilc, axis=1, keepdims=True)
    ilb = jnp.broadcast_to(ilc, (16, 128))
    il_kx = jnp.where(iota((16, 512), 0) == iota((16, 512), 1) >> 5, ilc, 0.0)
    il_kx = jnp.sum(il_kx, axis=0, keepdims=True)
    loads[1].wait()
    for g in range(2):
        il = il_kx[0:1, g * 256 : (g + 1) * 256]
        rows, cols = iota((16, 256), 0), iota((16, 256), 1)
        x = (cols & 31).astype(F32)
        up = jnp.exp((x - 31.0) * il)
        down = jnp.exp(-x * il) - jnp.exp((x - 2.0 * rest_x) * il)
        table = jnp.where(cols >> 5 == (rows & 7), jnp.where(rows < 8, up, down), 0.0)
        high, low = halves(table)
        for m in range(4):
            s = ctrl[m, g * 8 : (g + 1) * 8].reshape(256, 128)
            e = dot(high, s) + dot(low, s)
            lat_send[0, m, g * 8 : (g + 1) * 8, :] = e[0:8]
            lat_send[1, m, g * 8 : (g + 1) * 8, :] = e[8:16]

    pl.semaphore_wait(barrier, TILES - 1 + LAT * (Y * C - 1) + LON)
    lat_copies = []
    for d in range(1, LAT):
        copy = remote(
            lat_send.at[(a + d) // LAT], lat_recv.at[d - 1], lat_s.at[d - 1], lat_r.at[d - 1],
            (mem, (a + d) % LAT, b),
        )
        copy.start()
        lat_copies.append(copy)

    for g in range(2):
        il = il_kx[0:1, g * 256 : (g + 1) * 256]
        rows, cols = iota((256, 256), 0), iota((256, 256), 1)
        x1, x2 = (rows & 31).astype(F32), (cols & 31).astype(F32)
        near = jnp.exp(-jnp.abs(x1 - x2) * il)
        back = jnp.exp((x1 + x2 - 2.0 * rest_x) * il)
        high, low = halves(jnp.where(rows >> 5 == cols >> 5, near - back, 0.0))
        for m in range(4):
            s = ctrl[m, g * 8 : (g + 1) * 8].reshape(256, 128)
            out = dot(high, s) + dot(low, s)
            field[g * 8 : (g + 1) * 8, m * TX : (m + 1) * TX, :] = out.reshape(8, TX, TY)

    carry_l, carry_r = [0.0] * 4, [0.0] * 4
    for d in range(1, LAT):
        lat_copies[d - 1].wait_recv()
        left = jnp.where(a >= d, 1.0, 0.0)
        wl = jnp.exp(-32.0 * (d - 1) * ilb) * left
        wr = jnp.exp(-32.0 * (LAT - 1 - d) * ilb) * (1.0 - left)
        for m in range(4):
            got = lat_recv[d - 1, m]
            carry_l[m] = carry_l[m] + wl * got
            carry_r[m] = carry_r[m] + wr * got
    x = iota((TX, TY), 0).astype(F32)
    ly = iota((8, TY), 1).astype(F32)
    row8 = iota((8, TY), 0)
    for k in range(16):
        il = ilb[k : k + 1]
        ahead = jnp.exp(-(x + 1.0) * il) - jnp.exp((x - 1.0 - 2.0 * rest_x) * il)
        behind = jnp.exp((x - 32.0) * il)
        for m in range(4):
            here = slice(m * TX, (m + 1) * TX)
            field[k, here, :] = (
                field[k, here, :] + ahead * carry_l[m][k : k + 1] + behind * carry_r[m][k : k + 1]
            )
        up = jnp.exp((ly - 127.0) * il)
        down = jnp.exp(-ly * il) - jnp.exp((ly - 2.0 * rest_y) * il)
        th, tl = halves(jnp.where(row8 == 0, up, down))
        fh, fl = halves(field[k])
        e = dot_nt(th, fh) + dot_nt(th, fl) + dot_nt(tl, fh)
        lon_send[0, k : k + 1, :] = e[0:1]
        lon_send[1, k : k + 1, :] = e[1:2]
    lon_copies = []
    for d in range(1, LON):
        copy = remote(
            lon_send.at[(b + d) // LON], lon_recv.at[d - 1], lon_s.at[d - 1], lon_r.at[d - 1],
            (mem, a, (b + d) % LON),
        )
        copy.start()
        lon_copies.append(copy)

    for load in loads[2:5]:
        load.wait()
    t = tgt[...]
    rel = (((t >> 3) + (LAT - a)) & 3) * LON + (((t & 7) + (LON - b)) & 7)
    marks = jnp.where(iota((TILES, 512), 0) == rel, 1.0, 0.0)
    before = jnp.where(iota((512, 512), 0) < iota((512, 512), 1), 1.0, 0.0).astype(BF16)
    rank = jnp.sum(dot(marks.astype(BF16), before) * marks, axis=0, keepdims=True).astype(I32)
    slot = rel * 32 + rank
    chosen = jnp.where(iota((1024, 512), 0) == slot, 1.0, 0.0).astype(BF16)
    r32 = iota((32, 64), 0)
    level = (r32 >> 2) * 8 + c * 4 + (r32 & 3)
    own = jnp.where(iota((32, 64), 1) == level, 1.0, 0.0).astype(BF16)
    picked = dot(own, weights[...])
    place = col[...]
    r8 = iota((8, 512), 0)
    places = jnp.where(r8 == 0, (place >> 7).astype(F32), (place & 127).astype(F32))
    packed = dot_nt(jnp.concatenate([picked, places], 0).astype(BF16), chosen)
    spot = jnp.broadcast_to(packed[32:33] * 128.0 + packed[33:34], (8, 1024))
    group = iota((8, 128), 1) >> 5

    def turned(v, quarters):
        return pltpu.roll(v, 32 * (quarters % 4), 1) if quarters % 4 else v

    for k in range(TILES):
        block, j = slice(k // 4 * 128, k // 4 * 128 + 128), k % 4
        tile = turned(packed[0:8, block], -j)
        for g in range(1, 4):
            tile = jnp.where(group == g, turned(packed[8 * g : 8 * g + 8, block], g - j), tile)
        into = pk_send if k else pk_recv
        into[k, 0:8, :] = tile
        into[k, 8:9, :] = turned(spot[:, block], -j)[0:1]

    pk_copies = []
    for k in range(1, TILES):
        copy = remote(
            pk_send.at[k], pk_recv.at[k], pk_s.at[k - 1], pk_r.at[k - 1],
            (mem, (a + k // LON) % LAT, (b + k % LON) % LON),
        )
        copy.start()
        pk_copies.append(copy)

    y1, y2 = iota((TY, TY), 0).astype(F32), iota((TY, TY), 1).astype(F32)
    for k in range(16):
        il = ilb[k : k + 1]
        nh, nl = halves(
            jnp.exp(-jnp.abs(y1 - y2) * il) - jnp.exp((y1 + y2 - 2.0 * rest_y) * il)
        )
        fh, fl = halves(field[k])
        field[k] = dot(fh, nh) + dot(fl, nh) + dot(fh, nl)

    loads[5].wait()
    half = 0.5 * ilc
    sq = half * half
    gain = half * (1.0 - sq * (1.0 / 3.0 - sq * (2.0 / 15.0 - sq * (17.0 / 315.0))))
    scaled = modes[...] * (gain * (1.0 / math.sqrt(4 * ZH * Y * C - 1)))
    spread = jnp.where(iota((512, 64), 0) >> 3 == iota((512, 64), 1), 1.0, 0.0).astype(BF16)
    widen = jnp.where(iota((16, 128), 0) == iota((16, 128), 1) >> 3, 1.0, 0.0).astype(BF16)
    diagonal = (iota((512, 128), 0) & 7) == (iota((512, 128), 1) & 7)
    mh, ml = (
        jnp.where(diagonal, dot(spread, dot_tn(part, widen).astype(BF16)), 0.0).astype(BF16)
        for part in halves(scaled)
    )

    mhh = jnp.concatenate([mh, mh], 1)

    cl, cr = 0.0, 0.0
    for d in range(1, LON):
        lon_copies[d - 1].wait_recv()
        left = jnp.where(b >= d, 1.0, 0.0)
        got = lon_recv[d - 1]
        cl = cl + (jnp.exp(-128.0 * (d - 1) * ilb) * left) * got
        cr = cr + (jnp.exp(-128.0 * (LON - 1 - d) * ilb) * (1.0 - left)) * got
    for k in range(16):
        il = ilb[k : k + 1]
        ahead = jnp.exp(-(ly + 1.0) * il) - jnp.exp((ly - 1.0 - 2.0 * rest_y) * il)
        behind = jnp.exp((ly - 128.0) * il)
        ah, al = halves(jnp.where(row8 == 0, ahead, jnp.where(row8 == 1, behind, 0.0)))
        ch, co = halves(
            jnp.where(row8 == 0, cl[k : k + 1], jnp.where(row8 == 1, cr[k : k + 1], 0.0))
        )
        field[k] = field[k] + (dot_tn(ch, ah) + dot_tn(co, ah) + dot_tn(ch, al))

    loads[7].wait()
    core_copies = []
    for xb in range(4):
        acc = None
        for pair in range(2):
            rows = jnp.concatenate(
                [
                    field[:, m * TX + xb * 8 : m * TX + xb * 8 + 8, :].reshape(128, 128)
                    for m in (2 * pair, 2 * pair + 1)
                ],
                1,
            )
            fh, fl = halves(rows)
            prof = dot(mhh, jnp.concatenate([fh, fl], 0)) + dot(ml, fh)
            for n in range(2):
                p = pert[2 * pair + n, :, xb * 8 : xb * 8 + 8, :].astype(F32).reshape(512, 128)
                term = prof[:, n * 128 : n * 128 + 128] * p
                acc = term if acc is None else acc + term
        total[:, :, :, xb * 8 : xb * 8 + 8, :] = acc.reshape(8, 2, 4, 8, 128)
        part = pl.ds(xb * 8, 8)
        copy = remote(
            total.at[:, 1 - c, :, part, :], core_recv.at[:, :, part, :],
            core_s.at[xb], core_r.at[xb], (mem + 1 - 2 * c, a, b),
        )
        copy.start()
        core_copies.append(copy)

    for copy in core_copies:
        copy.wait_recv()
    whole = total[:, c] + core_recv[...]
    red1[...] = whole.reshape(2, 4, 4, TX, TY)
    y_copies = []
    for h, half in enumerate((1 - zh, zh)):
        for d in range(1, Y):
            yp = (y + d) % Y
            n = h * (Y - 1) + d - 1
            copy = remote(
                red1.at[half, yp], y_recv.at[n], y_s.at[n], y_r.at[n],
                ((zh * Y + yp) * C + c, a, b),
            )
            copy.start()
            y_copies.append(copy)

    lane = iota((8, 128), 1)
    r8 = iota((8, 128), 0)
    ends = jnp.where(
        (r8 == 0) & (lane == 0) | (r8 == 1) & (lane == 127), 1.0, 0.0
    ).astype(BF16)
    wh, wl = halves(whole.reshape(1024, 128))
    row_send[0] = red1[:, :, :, TX - 1, :].reshape(32, 128)
    row_send[1] = red1[:, :, :, 0, :].reshape(32, 128)
    edge_send[...] = (dot_nt(ends, wh) + dot_nt(ends, wl))[0:2]
    halo = []
    for s in range(2):
        step = 1 - 2 * s
        copy = remote(
            row_send.at[s], row_recv.at[s], row_s.at[s], row_r.at[s],
            (mem, (a + step + LAT) % LAT, b),
        )
        there, back = a + step, a - step
        halo.append((copy, (there >= 0) & (there < LAT), (back >= 0) & (back < LAT)))
    for i, da in enumerate((-1, 0, 1)):
        for j, db in enumerate((-1, 1)):
            copy = remote(
                edge_send, edge_recv.at[i, j], edge_s.at[i, j], edge_r.at[i, j],
                (mem, (a - da + LAT) % LAT, (b - db + LON) % LON),
            )
            at, bt, af, bf = a - da, b - db, a + da, b + db
            halo.append((
                copy,
                (at >= 0) & (at < LAT) & (bt >= 0) & (bt < LON),
                (af >= 0) & (af < LAT) & (bf >= 0) & (bf < LON),
            ))
    for copy, sends, _ in halo:
        pl.when(sends)(copy.start)

    w_all, p_all = [jnp.zeros((64, 128), F32)] * 4, jnp.zeros((8, 128), F32)
    g64 = iota((64, 128), 1) >> 5
    for da in range(LAT):
        for k in range(max(1, da * LON), (da + 1) * LON):
            pk_copies[k - 1].wait_recv()
        got = pk_recv[da * LON : (da + 1) * LON, 0:8, :].reshape(64, 128)
        w_all = [
            jnp.where(g64 == da, turned(got, da - g), w) for g, w in enumerate(w_all)
        ]
        p_all = jnp.where(
            group == da, turned(pk_recv[da * LON : (da + 1) * LON, 8, :], da), p_all
        )
    ys, xs = iota((TY, 128), 0), iota((TX, 128), 0)

    def blend(near, far, at):
        return jnp.where(at == near, 0.75, 0.0) + jnp.where(at == far, 0.25, 0.0)

    double = jnp.concatenate([wh, wl], 1)
    spots = []
    for db in range(LON):
        spot = p_all[db : db + 1].astype(I32)
        i, j = spot >> 8, spot & 255
        nx, ny = i >> 1, j >> 1
        fx, fy = nx + 2 * (i & 1) - 1, ny + 2 * (j & 1) - 1
        cols, rows = blend(ny, fy, ys).astype(BF16), blend(nx, fx, xs)
        inner = dot(double, jnp.concatenate([cols, cols], 0))
        inner = jnp.sum(inner.reshape(32, TX, 128) * rows[None], axis=1)
        around = [blend(ny, fy, -1), blend(ny, fy, TY), blend(nx, fx, -1), blend(nx, fx, TX)]
        spots.append((inner, cols, rows.astype(BF16), *around))

    for copy, _, gets in halo:
        pl.when(gets)(copy.wait_recv)
    beyond = jnp.concatenate([*halves(row_recv[0]), *halves(row_recv[1])], 0)
    z32, l32 = iota((32, 1024), 0), iota((32, 1024), 1)
    fold = jnp.where(iota((1024, TX), 0) & 31 == iota((1024, TX), 1), 1.0, 0.0).astype(BF16)

    def at_level(line, where):
        return jnp.where(where, line, 0.0)

    left, right = edge_recv[1, 0][1:2], edge_recv[1, 1][0:1]
    same = l32 >> 5 == z32
    beside = jnp.concatenate(
        [*halves(at_level(left, same)), *halves(at_level(right, same))], 0
    )
    beside = dot(beside, fold).astype(BF16)
    corner = [
        jnp.sum(at_level(edge_recv[i, j][1 - j : 2 - j], l32 == z32 * 32 + x), 1, keepdims=True)
        for i, x in ((0, TX - 1), (2, 0))
        for j in range(2)
    ]
    val_copies = []
    for db in range(LON):
        inner, cols, rows, west, east, north, south = spots[db]
        ud = dot(beyond, cols)
        lr = dot(beside, rows)
        up = ud[0:32] + ud[32:64] + corner[0] * west + corner[1] * east
        down = ud[64:96] + ud[96:128] + corner[2] * west + corner[3] * east
        inner = inner + (lr[0:32] + lr[32:64]) * west + (lr[64:96] + lr[96:128]) * east
        inner = inner + up * north + down * south
        w = jnp.concatenate([w[db * 8 : db * 8 + 8] for w in w_all], 0)
        val[db] = jnp.sum(inner * w, axis=0, keepdims=True)
        for zo in range(ZH):
            n = zo * LON + db
            if n:
                copy = remote(
                    val.at[db], val_recv.at[n], val_s.at[n - 1], val_r.at[n - 1],
                    ((mem + zo * Y * C) % (ZH * Y * C), a, (b - db + LON) % LON),
                )
                copy.start()
                val_copies.append(copy)

    for copy in y_copies[: Y - 1]:
        copy.wait_recv()
    red2[...] = red1[1 - zh, y] + y_recv[0] + y_recv[1] + y_recv[2]
    z_copy = remote(
        red2, z_recv, z_s.at[0], z_r.at[0],
        ((mem + Y * C) % (ZH * Y * C), a, b),
    )
    z_copy.start()

    val_recv[0] = val[0]
    for copy in val_copies:
        copy.wait_recv()
    for db in range(LON):
        vsum[db : db + 1, :] = val_recv[db] + val_recv[LON + db]
    both = vsum[...]
    kept = group == (iota((8, 128), 0) & 3)
    for da in range(LAT):
        mine = jnp.zeros((8, 128), F32)
        for g in range(4):
            mine = jnp.where(kept & (group == g), turned(both, g - da), mine)
        mine = jnp.sum(mine.reshape(2, 4, 128), axis=1)
        if da:
            last_send[da - 1] = mine
        else:
            last_send[LAT - 1] = mine
            last_recv[0] = mine
    last_copies = []
    for da in range(LAT):
        for d in range(Y * C):
            n = da * Y * C + d
            if n:
                copy = remote(
                    last_send.at[(da + LAT - 1) % LAT], last_recv.at[n],
                    last_s.at[n - 1], last_r.at[n - 1],
                    (zh * Y * C + (q + d) % (Y * C), (a + LAT - da) % LAT, b),
                )
                copy.start()
                last_copies.append(copy)
    for copy in y_copies[Y - 1 :]:
        copy.wait_recv()
    own = red1[zh, y] + y_recv[3] + y_recv[4] + y_recv[5]
    z_copy.wait_recv()
    inc_ref[...] = own + z_recv[...]
    inc_copy = pltpu.make_async_copy(inc_ref, inc_hbm, load_sem.at[9])
    inc_copy.start()
    for copy in last_copies:
        copy.wait_recv()
    table = []
    for da in range(LAT):
        block = last_recv[da * Y * C]
        for d in range(1, Y * C):
            block = block + last_recv[da * Y * C + d]
        table.append(block)
    table = jnp.concatenate(table, 0)
    marks = jnp.where(iota((8, 512), 0) == rel >> 2, 1.0, 0.0).astype(BF16)
    found = sum(dot_tn(part, marks) for part in thirds(table))
    here = iota((128, 512), 0) == (rel & 3) * 32 + rank
    equivalent = jnp.sum(jnp.where(here, found, 0.0), axis=0, keepdims=True)
    loads[6].wait()
    live = iota((1, 512), 1) < count[0]
    dep_ref[...] = jnp.where(live, innovation[...] - equivalent, 0.0)
    dep_copy = pltpu.make_async_copy(dep_ref, dep_hbm, load_sem.at[8])
    dep_copy.start()
    inc_copy.wait()
    dep_copy.wait()

    for copy in (*lat_copies, *lon_copies, *pk_copies, *core_copies, *y_copies, z_copy):
        copy.wait_send()
    for copy in (*val_copies, *last_copies):
        copy.wait_send()
    for copy, sends, _ in halo:
        pl.when(sends)(copy.wait_send)


def deliver(increment, departures, inc_hbm, dep_hbm, inc, dep, sems):
    pairs = ((increment, inc, inc_hbm), (departures, dep, dep_hbm))
    inward = [pltpu.make_async_copy(p[0], p[1], sems.at[n]) for n, p in enumerate(pairs)]
    outward = [pltpu.make_async_copy(p[1], p[2], sems.at[2 + n]) for n, p in enumerate(pairs)]
    for copy in inward:
        copy.start()
    for back, forth in zip(inward, outward):
        back.wait()
        forth.start()
    for copy in outward:
        copy.wait()


def per_device(
    perturbation, control, filter_length, modes, obs_weights, innovation, obs_tile,
    obs_column, obs_count,
):
    vmem = pl.BlockSpec(memory_space=pltpu.VMEM)
    hbm = pl.BlockSpec(memory_space=pltpu.HBM)
    smem = pl.BlockSpec(memory_space=pltpu.SMEM)
    f32 = lambda *shape: pltpu.VMEM(shape, F32)
    sem = lambda *shape: pltpu.SemaphoreType.DMA(shape)
    pairs = lambda *shape: [sem(*shape), sem(*shape)]
    increment, departures = pl.pallas_call(
        kernel,
        out_shape=(
            jax.ShapeDtypeStruct((4, TX, TY), F32),
            jax.ShapeDtypeStruct((1, 512), F32),
        ),
        in_specs=[hbm] * 6 + [smem] + [hbm] * 2,
        out_specs=(hbm, hbm),
        scratch_shapes=[
            f32(1, 16), f32(16, 64), pltpu.VMEM((64, 512), BF16), f32(1, 512),
            pltpu.VMEM((1, 512), I32), pltpu.VMEM((1, 512), I32),
            pltpu.VMEM((4, 16, TX, TY), BF16), pltpu.VMEM((4, 64, TX, TY), BF16),
            f32(16, 128, TY),
            f32(2, 4, 16, TY), f32(LAT - 1, 4, 16, TY),
            f32(2, 16, 128), f32(LON - 1, 16, 128),
            f32(TILES, 9, 128), f32(TILES, 9, 128),
            f32(8, 2, 4, TX, TY), f32(8, 4, TX, TY),
            f32(2, 4, 4, TX, TY), f32(2 * (Y - 1), 4, TX, TY),
            f32(4, TX, TY), f32(4, TX, TY),
            f32(2, 32, 128), f32(2, 32, 128), f32(2, 1024), f32(3, 2, 2, 1024),
            f32(LON, 1, 128), f32(ZH * LON, 1, 128), f32(8, 128),
            f32(LAT, 2, 128), f32(LAT * Y * C, 2, 128),
            f32(4, TX, TY), f32(1, 512),
            sem(10), *pairs(LAT - 1), *pairs(LON - 1), *pairs(TILES - 1), *pairs(4),
            *pairs(2 * (Y - 1)), *pairs(1), *pairs(2), *pairs(3, 2), *pairs(ZH * LON - 1),
            *pairs(LAT * Y * C - 1),
        ],
        compiler_params=pltpu.CompilerParams(
            collective_id=0, has_side_effects=True, vmem_limit_bytes=60_000_000
        ),
        name="hybrid",
    )(
        filter_length.reshape(1, 16),
        modes.T,
        obs_weights.T,
        innovation.reshape(1, 512),
        obs_tile.reshape(1, 512),
        obs_column.reshape(1, 512),
        obs_count,
        control,
        perturbation,
    )
    increment, departures = pl.pallas_call(
        deliver,
        out_shape=(
            jax.ShapeDtypeStruct((4, TX, TY), F32),
            jax.ShapeDtypeStruct((1, 512), F32),
        ),
        in_specs=[hbm] * 2,
        out_specs=(hbm, hbm),
        scratch_shapes=[f32(4, TX, TY), f32(1, 512), sem(4)],
        name="deliver",
    )(increment, departures)
    return increment, departures.reshape(512)


def solution(mesh):
    placed = (
        P("mem", None, "lat", "lon"),
        P("mem", None, "lat", "lon"),
        P(),
        P(),
        P(("lat", "lon"), None),
        P(("lat", "lon")),
        P(("lat", "lon"), None),
        P(("lat", "lon")),
        P(("lat", "lon")),
    )
    return jax.shard_map(
        per_device,
        mesh=mesh,
        in_specs=placed,
        out_specs=(P("mem", "lat", "lon"), P(("lat", "lon"))),
        check_vma=False,
    )
```

```python
import math

import jax
import jax.numpy as jnp
from jax import lax
from jax.experimental import pallas as pl
from jax.experimental.pallas import tpu as pltpu
from jax.sharding import PartitionSpec as P

F32, BF16, I32 = jnp.float32, jnp.bfloat16, jnp.int32
MESH = pl.DeviceIdType.MESH
ZH, Y, C = 2, 4, 2
LAT, LON = 4, 8
NX, NY, TX, TY = 128, 1024, 32, 128
TILES = LAT * LON


def iota(shape, dim):
    return lax.broadcasted_iota(I32, shape, dim)


def halves(v):
    high = v.astype(BF16)
    return high, (v - high.astype(F32)).astype(BF16)


def thirds(v):
    high, rest = v.astype(BF16), v - v.astype(BF16).astype(F32)
    return (high, *halves(rest))


def dot(a, b):
    return lax.dot_general(a, b, (((1,), (0,)), ((), ())), preferred_element_type=F32)


def dot_nt(a, b):
    return lax.dot_general(a, b, (((1,), (1,)), ((), ())), preferred_element_type=F32)


def dot_tn(a, b):
    return lax.dot_general(a, b, (((0,), (0,)), ((), ())), preferred_element_type=F32)


def kernel(
    length_hbm, modes_hbm, weights_hbm, innovation_hbm, tgt_hbm, col_hbm, count, ctrl_hbm, pert_hbm,
    inc_hbm, dep_hbm,
    length, modes, weights, innovation, tgt, col,
    ctrl, pert, field, lat_send, lat_recv, lon_send, lon_recv, pk_send, pk_recv,
    pk_all, w_all, blended, total, core_recv, red1, y_recv, red2, z_recv,
    row_send, row_recv, edge_send, edge_recv, val, val_recv, vsum, last_send, last_recv, inc_ref, dep_ref,
    load_sem, lat_s, lat_r, lon_s, lon_r, pk_s, pk_r, share_s, share_r, core_s, core_r, y_s, y_r, z_s, z_r,
    row_s, row_r, edge_s, edge_r, val_s, val_r, last_s, last_r,
):
    mem, a, b = (lax.axis_index(n) for n in ("mem", "lat", "lon"))
    zh, y, c = mem // (Y * C), (mem // C) % Y, mem % C
    q = y * C + c

    def remote(src, dst, s, r, dev):
        return pltpu.make_async_remote_copy(
            src_ref=src, dst_ref=dst, send_sem=s, recv_sem=r, device_id=dev, device_id_type=MESH
        )

    loads = [
        pltpu.make_async_copy(src, dst, load_sem.at[n])
        for n, (src, dst) in enumerate((
            (length_hbm, length), (ctrl_hbm, ctrl), (tgt_hbm, tgt), (col_hbm, col),
            (weights_hbm, weights), (modes_hbm, modes), (innovation_hbm, innovation),
            (pert_hbm, pert),
        ))
    ]
    for load in loads:
        load.start()
    row_recv[...] = jnp.zeros_like(row_recv)
    edge_recv[...] = jnp.zeros_like(edge_recv)

    barrier = pltpu.get_barrier_semaphore()

    def greet(dev):
        pl.semaphore_signal(barrier, inc=1, device_id=dev, device_id_type=MESH)

    for d in range(1, TILES):
        greet((mem, (a + d // LON) % LAT, (b + d % LON) % LON))
    for d in range(1, Y * C):
        greet((zh * Y * C + (q + d) % (Y * C), a, b))
    for d in range(LON):
        greet(((mem + Y * C) % (ZH * Y * C), a, (b + d) % LON))
    for da in range(1, LAT):
        for d in range(1, Y * C):
            greet((zh * Y * C + (q + d) % (Y * C), (a + da) % LAT, b))

    rest_x = (NX - TX * a).astype(F32)
    rest_y = (NY - TY * b).astype(F32)
    loads[0].wait()
    ilc = jnp.where(iota((16, 16), 0) == iota((16, 16), 1), 1.0 / length[...], 0.0)
    ilc = jnp.sum(ilc, axis=1, keepdims=True)
    ilb = jnp.broadcast_to(ilc, (16, 128))
    il_kx = jnp.where(iota((16, 512), 0) == iota((16, 512), 1) >> 5, ilc, 0.0)
    il_kx = jnp.sum(il_kx, axis=0, keepdims=True)
    loads[1].wait()
    for g in range(2):
        il = il_kx[0:1, g * 256 : (g + 1) * 256]
        rows, cols = iota((16, 256), 0), iota((16, 256), 1)
        x = (cols & 31).astype(F32)
        up = jnp.exp((x - 31.0) * il)
        down = jnp.exp(-x * il) - jnp.exp((x - 2.0 * rest_x) * il)
        table = jnp.where(cols >> 5 == (rows & 7), jnp.where(rows < 8, up, down), 0.0)
        high, low = halves(table)
        for m in range(4):
            s = ctrl[m, g * 8 : (g + 1) * 8].reshape(256, 128)
            e = dot(high, s) + dot(low, s)
            lat_send[0, m, g * 8 : (g + 1) * 8, :] = e[0:8]
            lat_send[1, m, g * 8 : (g + 1) * 8, :] = e[8:16]

    pl.semaphore_wait(barrier, TILES - 1 + LAT * (Y * C - 1) + LON)
    lat_copies = []
    for d in range(1, LAT):
        copy = remote(
            lat_send.at[(a + d) // LAT], lat_recv.at[d - 1], lat_s.at[d - 1], lat_r.at[d - 1],
            (mem, (a + d) % LAT, b),
        )
        copy.start()
        lat_copies.append(copy)

    for load in loads[2:5]:
        load.wait()
    t = tgt[...]
    rel = (((t >> 3) + (LAT - a)) & 3) * LON + (((t & 7) + (LON - b)) & 7)
    marks = jnp.where(iota((TILES, 512), 0) == rel, 1.0, 0.0)
    before = jnp.where(iota((512, 512), 0) < iota((512, 512), 1), 1.0, 0.0).astype(BF16)
    rank = jnp.sum(dot(marks.astype(BF16), before) * marks, axis=0, keepdims=True).astype(I32)
    slot = rel * 32 + rank
    chosen = jnp.where(iota((1024, 512), 0) == slot, 1.0, 0.0).astype(BF16)
    share = y * 8 + iota((8, 64), 0)
    level = (share >> 2) * 8 + c * 4 + (share & 3)
    own = jnp.where(iota((8, 64), 1) == level, 1.0, 0.0).astype(BF16)
    picked = dot(own, weights[...])
    place = col[...]
    r8 = iota((8, 512), 0)
    places = jnp.where(r8 == 0, (place >> 7).astype(F32), (place & 127).astype(F32))
    packed = dot_nt(jnp.concatenate([picked, places], 0).astype(BF16), chosen)
    spot = jnp.broadcast_to(packed[8:9] * 128.0 + packed[9:10], (8, 1024))
    group = iota((8, 128), 1) >> 5
    kept = group == (iota((8, 128), 0) & 3)

    def turned(v, quarters):
        return pltpu.roll(v, 32 * (quarters % 4), 1) if quarters % 4 else v

    for k in range(TILES):
        block, j = slice(k // 4 * 128, k // 4 * 128 + 128), k % 4
        tile = jnp.zeros((8, 128), F32)
        for g in range(4):
            tile = jnp.where(kept & (group == g), turned(packed[0:8, block], g - j), tile)
        into = pk_send if k else pk_recv
        into[k, 0:2, :] = jnp.sum(tile.reshape(2, 4, 128), axis=1)
        into[k, 2:3, :] = turned(spot[:, block], -j)[0:1]

    pk_copies = []
    for k in range(1, TILES):
        copy = remote(
            pk_send.at[k], pk_recv.at[k], pk_s.at[k - 1], pk_r.at[k - 1],
            (mem, (a + k // LON) % LAT, (b + k % LON) % LON),
        )
        copy.start()
        pk_copies.append(copy)

    for g in range(2):
        il = il_kx[0:1, g * 256 : (g + 1) * 256]
        rows, cols = iota((256, 256), 0), iota((256, 256), 1)
        x1, x2 = (rows & 31).astype(F32), (cols & 31).astype(F32)
        near = jnp.exp(-jnp.abs(x1 - x2) * il)
        back = jnp.exp((x1 + x2 - 2.0 * rest_x) * il)
        high, low = halves(jnp.where(rows >> 5 == cols >> 5, near - back, 0.0))
        for m in range(4):
            s = ctrl[m, g * 8 : (g + 1) * 8].reshape(256, 128)
            out = dot(high, s) + dot(low, s)
            field[g * 8 : (g + 1) * 8, m * TX : (m + 1) * TX, :] = out.reshape(8, TX, TY)

    carry_l, carry_r = [0.0] * 4, [0.0] * 4
    for d in range(1, LAT):
        lat_copies[d - 1].wait_recv()
        left = jnp.where(a >= d, 1.0, 0.0)
        wl = jnp.exp(-32.0 * (d - 1) * ilb) * left
        wr = jnp.exp(-32.0 * (LAT - 1 - d) * ilb) * (1.0 - left)
        for m in range(4):
            got = lat_recv[d - 1, m]
            carry_l[m] = carry_l[m] + wl * got
            carry_r[m] = carry_r[m] + wr * got
    x = iota((TX, TY), 0).astype(F32)
    ly = iota((8, TY), 1).astype(F32)
    row8 = iota((8, TY), 0)
    for k in range(16):
        il = ilb[k : k + 1]
        ahead = jnp.exp(-(x + 1.0) * il) - jnp.exp((x - 1.0 - 2.0 * rest_x) * il)
        behind = jnp.exp((x - 32.0) * il)
        for m in range(4):
            here = slice(m * TX, (m + 1) * TX)
            field[k, here, :] = (
                field[k, here, :] + ahead * carry_l[m][k : k + 1] + behind * carry_r[m][k : k + 1]
            )
        up = jnp.exp((ly - 127.0) * il)
        down = jnp.exp(-ly * il) - jnp.exp((ly - 2.0 * rest_y) * il)
        th, tl = halves(jnp.where(row8 == 0, up, down))
        fh, fl = halves(field[k])
        e = dot_nt(th, fh) + dot_nt(th, fl) + dot_nt(tl, fh)
        lon_send[0, k : k + 1, :] = e[0:1]
        lon_send[1, k : k + 1, :] = e[1:2]
    lon_copies = []
    for d in range(1, LON):
        copy = remote(
            lon_send.at[(b + d) // LON], lon_recv.at[d - 1], lon_s.at[d - 1], lon_r.at[d - 1],
            (mem, a, (b + d) % LON),
        )
        copy.start()
        lon_copies.append(copy)

    y1, y2 = iota((TY, TY), 0).astype(F32), iota((TY, TY), 1).astype(F32)
    for k in range(16):
        il = ilb[k : k + 1]
        nh, nl = halves(
            jnp.exp(-jnp.abs(y1 - y2) * il) - jnp.exp((y1 + y2 - 2.0 * rest_y) * il)
        )
        fh, fl = halves(field[k])
        field[k] = dot(fh, nh) + dot(fl, nh) + dot(fh, nl)

    loads[5].wait()
    half = 0.5 * ilc
    sq = half * half
    gain = half * (1.0 - sq * (1.0 / 3.0 - sq * (2.0 / 15.0 - sq * (17.0 / 315.0))))
    scaled = modes[...] * (gain * (1.0 / math.sqrt(4 * ZH * Y * C - 1)))
    spread = jnp.where(iota((512, 64), 0) >> 3 == iota((512, 64), 1), 1.0, 0.0).astype(BF16)
    widen = jnp.where(iota((16, 128), 0) == iota((16, 128), 1) >> 3, 1.0, 0.0).astype(BF16)
    diagonal = (iota((512, 128), 0) & 7) == (iota((512, 128), 1) & 7)
    mh, ml = (
        jnp.where(diagonal, dot(spread, dot_tn(part, widen).astype(BF16)), 0.0).astype(BF16)
        for part in halves(scaled)
    )

    mhh = jnp.concatenate([mh, mh], 1)

    cl, cr = 0.0, 0.0
    for d in range(1, LON):
        lon_copies[d - 1].wait_recv()
        left = jnp.where(b >= d, 1.0, 0.0)
        got = lon_recv[d - 1]
        cl = cl + (jnp.exp(-128.0 * (d - 1) * ilb) * left) * got
        cr = cr + (jnp.exp(-128.0 * (LON - 1 - d) * ilb) * (1.0 - left)) * got
    for k in range(16):
        il = ilb[k : k + 1]
        ahead = jnp.exp(-(ly + 1.0) * il) - jnp.exp((ly - 1.0 - 2.0 * rest_y) * il)
        behind = jnp.exp((ly - 128.0) * il)
        ah, al = halves(jnp.where(row8 == 0, ahead, jnp.where(row8 == 1, behind, 0.0)))
        ch, co = halves(
            jnp.where(row8 == 0, cl[k : k + 1], jnp.where(row8 == 1, cr[k : k + 1], 0.0))
        )
        field[k] = field[k] + (dot_tn(ch, ah) + dot_tn(co, ah) + dot_tn(ch, al))

    for copy in pk_copies:
        copy.wait_recv()
    share_copies = []
    for d in range(1, Y):
        copy = remote(
            pk_recv, pk_all.at[d - 1], share_s.at[d - 1], share_r.at[d - 1],
            ((zh * Y + (y + d) % Y) * C + c, a, b),
        )
        copy.start()
        share_copies.append(copy)

    loads[7].wait()
    core_copies = []
    for xb in range(4):
        acc = None
        for pair in range(2):
            rows = jnp.concatenate(
                [
                    field[:, m * TX + xb * 8 : m * TX + xb * 8 + 8, :].reshape(128, 128)
                    for m in (2 * pair, 2 * pair + 1)
                ],
                1,
            )
            fh, fl = halves(rows)
            prof = dot(mhh, jnp.concatenate([fh, fl], 0)) + dot(ml, fh)
            for n in range(2):
                p = pert[2 * pair + n, :, xb * 8 : xb * 8 + 8, :].astype(F32).reshape(512, 128)
                term = prof[:, n * 128 : n * 128 + 128] * p
                acc = term if acc is None else acc + term
        total[:, :, :, xb * 8 : xb * 8 + 8, :] = acc.reshape(8, 2, 4, 8, 128)
        part = pl.ds(xb * 8, 8)
        copy = remote(
            total.at[:, 1 - c, :, part, :], core_recv.at[:, :, part, :],
            core_s.at[xb], core_r.at[xb], (mem + 1 - 2 * c, a, b),
        )
        copy.start()
        core_copies.append(copy)

    for copy in core_copies:
        copy.wait_recv()
    whole = total[:, c] + core_recv[...]
    red1[...] = whole.reshape(2, 4, 4, TX, TY)
    y_copies = []
    for h, half in enumerate((1 - zh, zh)):
        for d in range(1, Y):
            yp = (y + d) % Y
            n = h * (Y - 1) + d - 1
            copy = remote(
                red1.at[half, yp], y_recv.at[n], y_s.at[n], y_r.at[n],
                ((zh * Y + yp) * C + c, a, b),
            )
            copy.start()
            y_copies.append(copy)

    lane = iota((8, 128), 1)
    r8 = iota((8, 128), 0)
    ends = jnp.where(
        (r8 == 0) & (lane == 0) | (r8 == 1) & (lane == 127), 1.0, 0.0
    ).astype(BF16)
    wh, wl = halves(whole.reshape(1024, 128))
    row_send[0] = red1[:, :, :, TX - 1, :].reshape(32, 128)
    row_send[1] = red1[:, :, :, 0, :].reshape(32, 128)
    edge_send[...] = (dot_nt(ends, wh) + dot_nt(ends, wl))[0:2]
    halo = []
    for s in range(2):
        step = 1 - 2 * s
        copy = remote(
            row_send.at[s], row_recv.at[s], row_s.at[s], row_r.at[s],
            (mem, (a + step + LAT) % LAT, b),
        )
        there, back = a + step, a - step
        halo.append((copy, (there >= 0) & (there < LAT), (back >= 0) & (back < LAT)))
    for i, da in enumerate((-1, 0, 1)):
        for j, db in enumerate((-1, 1)):
            copy = remote(
                edge_send, edge_recv.at[i, j], edge_s.at[i, j], edge_r.at[i, j],
                (mem, (a - da + LAT) % LAT, (b - db + LON) % LON),
            )
            at, bt, af, bf = a - da, b - db, a + da, b + db
            halo.append((
                copy,
                (at >= 0) & (at < LAT) & (bt >= 0) & (bt < LON),
                (af >= 0) & (af < LAT) & (bf >= 0) & (bf < LON),
            ))
    for copy, sends, _ in halo:
        pl.when(sends)(copy.start)

    p_all = jnp.zeros((8, 128), F32)
    for da in range(LAT):
        got = pk_recv[da * LON : (da + 1) * LON, 2, :]
        p_all = jnp.where(group == da, turned(got, da), p_all)
    ys, xs = iota((TY, 128), 0), iota((TX, 128), 0)

    def blend(near, far, at):
        return jnp.where(at == near, 0.75, 0.0) + jnp.where(at == far, 0.25, 0.0)

    double = jnp.concatenate([wh, wl], 1)
    spots = []
    for db in range(LON):
        spot = p_all[db : db + 1].astype(I32)
        i, j = spot >> 8, spot & 255
        nx, ny = i >> 1, j >> 1
        fx, fy = nx + 2 * (i & 1) - 1, ny + 2 * (j & 1) - 1
        cols, rows = blend(ny, fy, ys).astype(BF16), blend(nx, fx, xs)
        inner = dot(double, jnp.concatenate([cols, cols], 0))
        inner = jnp.sum(inner.reshape(32, TX, 128) * rows[None], axis=1)
        around = [blend(ny, fy, -1), blend(ny, fy, TY), blend(nx, fx, -1), blend(nx, fx, TX)]
        spots.append((inner, cols, rows.astype(BF16), *around))

    for d in range(Y):
        if d:
            share_copies[d - 1].wait_recv()
        source = pk_all.at[d - 1] if d else pk_recv
        for r in range(8):
            w = jnp.zeros((8, 128), F32)
            for da in range(LAT):
                got = source[da * LON : (da + 1) * LON, r // 4, :]
                w = jnp.where(group == da, turned(got, da - r % 4), w)
            w_all[d, :, r, :] = w

    for copy, _, gets in halo:
        pl.when(gets)(copy.wait_recv)
    beyond = jnp.concatenate([*halves(row_recv[0]), *halves(row_recv[1])], 0)
    z32, l32 = iota((32, 1024), 0), iota((32, 1024), 1)
    fold = jnp.where(iota((1024, TX), 0) & 31 == iota((1024, TX), 1), 1.0, 0.0).astype(BF16)

    def at_level(line, where):
        return jnp.where(where, line, 0.0)

    left, right = edge_recv[1, 0][1:2], edge_recv[1, 1][0:1]
    same = l32 >> 5 == z32
    beside = jnp.concatenate(
        [*halves(at_level(left, same)), *halves(at_level(right, same))], 0
    )
    beside = dot(beside, fold).astype(BF16)
    corner = [
        jnp.sum(at_level(edge_recv[i, j][1 - j : 2 - j], l32 == z32 * 32 + x), 1, keepdims=True)
        for i, x in ((0, TX - 1), (2, 0))
        for j in range(2)
    ]
    val_copies = []
    for db in range(LON):
        inner, cols, rows, west, east, north, south = spots[db]
        ud = dot(beyond, cols)
        lr = dot(beside, rows)
        up = ud[0:32] + ud[32:64] + corner[0] * west + corner[1] * east
        down = ud[64:96] + ud[96:128] + corner[2] * west + corner[3] * east
        inner = inner + (lr[0:32] + lr[32:64]) * west + (lr[64:96] + lr[96:128]) * east
        inner = inner + up * north + down * south
        blended[db] = inner.reshape(Y, 8, 128)
        parts = [w_all[d, db] * blended[db, (y + Y - d) % Y] for d in range(Y)]
        val[db] = jnp.sum(sum(parts), axis=0, keepdims=True)
        for zo in range(ZH):
            n = zo * LON + db
            if n:
                copy = remote(
                    val.at[db], val_recv.at[n], val_s.at[n - 1], val_r.at[n - 1],
                    ((mem + zo * Y * C) % (ZH * Y * C), a, (b - db + LON) % LON),
                )
                copy.start()
                val_copies.append(copy)

    for copy in y_copies[: Y - 1]:
        copy.wait_recv()
    red2[...] = red1[1 - zh, y] + y_recv[0] + y_recv[1] + y_recv[2]
    z_copy = remote(
        red2, z_recv, z_s.at[0], z_r.at[0],
        ((mem + Y * C) % (ZH * Y * C), a, b),
    )
    z_copy.start()

    val_recv[0] = val[0]
    for copy in val_copies:
        copy.wait_recv()
    for db in range(LON):
        vsum[db : db + 1, :] = val_recv[db] + val_recv[LON + db]
    both = vsum[...]
    for da in range(LAT):
        mine = jnp.zeros((8, 128), F32)
        for g in range(4):
            mine = jnp.where(kept & (group == g), turned(both, g - da), mine)
        mine = jnp.sum(mine.reshape(2, 4, 128), axis=1)
        if da:
            last_send[da - 1] = mine
        else:
            last_send[LAT - 1] = mine
            last_recv[0] = mine
    last_copies = []
    for da in range(LAT):
        for d in range(Y * C):
            n = da * Y * C + d
            if n:
                copy = remote(
                    last_send.at[(da + LAT - 1) % LAT], last_recv.at[n],
                    last_s.at[n - 1], last_r.at[n - 1],
                    (zh * Y * C + (q + d) % (Y * C), (a + LAT - da) % LAT, b),
                )
                copy.start()
                last_copies.append(copy)
    for copy in y_copies[Y - 1 :]:
        copy.wait_recv()
    own = red1[zh, y] + y_recv[3] + y_recv[4] + y_recv[5]
    z_copy.wait_recv()
    inc_ref[...] = own + z_recv[...]
    inc_copy = pltpu.make_async_copy(inc_ref, inc_hbm, load_sem.at[9])
    inc_copy.start()
    for copy in last_copies:
        copy.wait_recv()
    table = []
    for da in range(LAT):
        block = last_recv[da * Y * C]
        for d in range(1, Y * C):
            block = block + last_recv[da * Y * C + d]
        table.append(block)
    table = jnp.concatenate(table, 0)
    marks = jnp.where(iota((8, 512), 0) == rel >> 2, 1.0, 0.0).astype(BF16)
    found = sum(dot_tn(part, marks) for part in thirds(table))
    here = iota((128, 512), 0) == (rel & 3) * 32 + rank
    equivalent = jnp.sum(jnp.where(here, found, 0.0), axis=0, keepdims=True)
    loads[6].wait()
    live = iota((1, 512), 1) < count[0]
    dep_ref[...] = jnp.where(live, innovation[...] - equivalent, 0.0)
    dep_copy = pltpu.make_async_copy(dep_ref, dep_hbm, load_sem.at[8])
    dep_copy.start()
    inc_copy.wait()
    dep_copy.wait()

    for copy in (*lat_copies, *lon_copies, *pk_copies, *core_copies, *y_copies, z_copy):
        copy.wait_send()
    for copy in (*share_copies, *val_copies, *last_copies):
        copy.wait_send()
    for copy, sends, _ in halo:
        pl.when(sends)(copy.wait_send)


def deliver(increment, departures, inc_hbm, dep_hbm, inc, dep, sems):
    pairs = ((increment, inc, inc_hbm), (departures, dep, dep_hbm))
    inward = [pltpu.make_async_copy(p[0], p[1], sems.at[n]) for n, p in enumerate(pairs)]
    outward = [pltpu.make_async_copy(p[1], p[2], sems.at[2 + n]) for n, p in enumerate(pairs)]
    for copy in inward:
        copy.start()
    for back, forth in zip(inward, outward):
        back.wait()
        forth.start()
    for copy in outward:
        copy.wait()


def per_device(
    perturbation, control, filter_length, modes, obs_weights, innovation, obs_tile,
    obs_column, obs_count,
):
    vmem = pl.BlockSpec(memory_space=pltpu.VMEM)
    hbm = pl.BlockSpec(memory_space=pltpu.HBM)
    smem = pl.BlockSpec(memory_space=pltpu.SMEM)
    f32 = lambda *shape: pltpu.VMEM(shape, F32)
    sem = lambda *shape: pltpu.SemaphoreType.DMA(shape)
    pairs = lambda *shape: [sem(*shape), sem(*shape)]
    increment, departures = pl.pallas_call(
        kernel,
        out_shape=(
            jax.ShapeDtypeStruct((4, TX, TY), F32),
            jax.ShapeDtypeStruct((1, 512), F32),
        ),
        in_specs=[hbm] * 6 + [smem] + [hbm] * 2,
        out_specs=(hbm, hbm),
        scratch_shapes=[
            f32(1, 16), f32(16, 64), pltpu.VMEM((64, 512), BF16), f32(1, 512),
            pltpu.VMEM((1, 512), I32), pltpu.VMEM((1, 512), I32),
            pltpu.VMEM((4, 16, TX, TY), BF16), pltpu.VMEM((4, 64, TX, TY), BF16),
            f32(16, 128, TY),
            f32(2, 4, 16, TY), f32(LAT - 1, 4, 16, TY),
            f32(2, 16, 128), f32(LON - 1, 16, 128),
            f32(TILES, 3, 128), f32(TILES, 3, 128),
            f32(Y - 1, TILES, 3, 128), f32(Y, LON, 8, 128), f32(LON, Y, 8, 128),
            f32(8, 2, 4, TX, TY), f32(8, 4, TX, TY),
            f32(2, 4, 4, TX, TY), f32(2 * (Y - 1), 4, TX, TY),
            f32(4, TX, TY), f32(4, TX, TY),
            f32(2, 32, 128), f32(2, 32, 128), f32(2, 1024), f32(3, 2, 2, 1024),
            f32(LON, 1, 128), f32(ZH * LON, 1, 128), f32(8, 128),
            f32(LAT, 2, 128), f32(LAT * Y * C, 2, 128),
            f32(4, TX, TY), f32(1, 512),
            sem(10), *pairs(LAT - 1), *pairs(LON - 1), *pairs(TILES - 1),
            *pairs(Y - 1), *pairs(4),
            *pairs(2 * (Y - 1)), *pairs(1), *pairs(2), *pairs(3, 2), *pairs(ZH * LON - 1),
            *pairs(LAT * Y * C - 1),
        ],
        compiler_params=pltpu.CompilerParams(
            collective_id=0, has_side_effects=True, vmem_limit_bytes=60_000_000
        ),
        name="hybrid",
    )(
        filter_length.reshape(1, 16),
        modes.T,
        obs_weights.T,
        innovation.reshape(1, 512),
        obs_tile.reshape(1, 512),
        obs_column.reshape(1, 512),
        obs_count,
        control,
        perturbation,
    )
    increment, departures = pl.pallas_call(
        deliver,
        out_shape=(
            jax.ShapeDtypeStruct((4, TX, TY), F32),
            jax.ShapeDtypeStruct((1, 512), F32),
        ),
        in_specs=[hbm] * 2,
        out_specs=(hbm, hbm),
        scratch_shapes=[f32(4, TX, TY), f32(1, 512), sem(4)],
        name="deliver",
    )(increment, departures)
    return increment, departures.reshape(512)


def solution(mesh):
    placed = (
        P("mem", None, "lat", "lon"),
        P("mem", None, "lat", "lon"),
        P(),
        P(),
        P(("lat", "lon"), None),
        P(("lat", "lon")),
        P(("lat", "lon"), None),
        P(("lat", "lon")),
        P(("lat", "lon")),
    )
    return jax.shard_map(
        per_device,
        mesh=mesh,
        in_specs=placed,
        out_specs=(P("mem", "lat", "lon"), P(("lat", "lon"))),
        check_vma=False,
    )
```

```python
import math

import jax
import jax.numpy as jnp
from jax import lax
from jax.experimental import pallas as pl
from jax.experimental.pallas import tpu as pltpu
from jax.sharding import PartitionSpec as P

F32, BF16, I32 = jnp.float32, jnp.bfloat16, jnp.int32
MESH = pl.DeviceIdType.MESH
ZH, Y, C = 2, 4, 2
LAT, LON = 4, 8
NX, NY, TX, TY = 128, 1024, 32, 128
TILES = LAT * LON


def iota(shape, dim):
    return lax.broadcasted_iota(I32, shape, dim)


def halves(v):
    high = v.astype(BF16)
    return high, (v - high.astype(F32)).astype(BF16)


def thirds(v):
    high, rest = v.astype(BF16), v - v.astype(BF16).astype(F32)
    return (high, *halves(rest))


def dot(a, b):
    return lax.dot_general(a, b, (((1,), (0,)), ((), ())), preferred_element_type=F32)


def dot_nt(a, b):
    return lax.dot_general(a, b, (((1,), (1,)), ((), ())), preferred_element_type=F32)


def dot_tn(a, b):
    return lax.dot_general(a, b, (((0,), (0,)), ((), ())), preferred_element_type=F32)


def kernel(
    length_hbm, modes_hbm, weights_hbm, innovation_hbm, tgt_hbm, col_hbm, count, ctrl_hbm, pert_hbm,
    inc_hbm, dep_hbm,
    length, modes, weights, innovation, tgt, col,
    ctrl, pert, field, lat_send, lat_recv, lon_send, lon_recv, pk_send, pk_recv,
    pk_all, w_all, blended, total, core_recv, red1, y_recv, red2, z_recv,
    row_send, row_recv, edge_send, edge_recv, val, val_recv, vsum, last_send, last_recv, inc_ref, dep_ref,
    load_sem, lat_s, lat_r, lon_s, lon_r, pk_s, pk_r, share_s, share_r, core_s, core_r, y_s, y_r, z_s, z_r,
    row_s, row_r, edge_s, edge_r, val_s, val_r, last_s, last_r,
):
    mem, a, b = (lax.axis_index(n) for n in ("mem", "lat", "lon"))
    zh, y, c = mem // (Y * C), (mem // C) % Y, mem % C
    q = y * C + c

    def remote(src, dst, s, r, dev):
        return pltpu.make_async_remote_copy(
            src_ref=src, dst_ref=dst, send_sem=s, recv_sem=r, device_id=dev, device_id_type=MESH
        )

    loads = [
        pltpu.make_async_copy(src, dst, load_sem.at[n])
        for n, (src, dst) in enumerate((
            (length_hbm, length), (ctrl_hbm, ctrl), (tgt_hbm, tgt), (col_hbm, col),
            (weights_hbm, weights), (modes_hbm, modes), (innovation_hbm, innovation),
            (pert_hbm, pert),
        ))
    ]
    for load in loads:
        load.start()
    row_recv[...] = jnp.zeros_like(row_recv)
    edge_recv[...] = jnp.zeros_like(edge_recv)

    barrier = pltpu.get_barrier_semaphore()

    def greet(dev):
        pl.semaphore_signal(barrier, inc=1, device_id=dev, device_id_type=MESH)

    for d in range(1, TILES):
        greet((mem, (a + d // LON) % LAT, (b + d % LON) % LON))
    for d in range(1, Y * C):
        greet((zh * Y * C + (q + d) % (Y * C), a, b))
    for d in range(LON):
        greet(((mem + Y * C) % (ZH * Y * C), a, (b + d) % LON))
    for da in (LAT - 1, 0, 1):
        for db in (LON - 1, 1):
            greet((mem + 1 - 2 * c, (a + da) % LAT, (b + db) % LON))
    for da in range(1, LAT):
        for d in range(1, Y * C):
            greet((zh * Y * C + (q + d) % (Y * C), (a + da) % LAT, b))

    rest_x = (NX - TX * a).astype(F32)
    rest_y = (NY - TY * b).astype(F32)
    loads[0].wait()
    ilc = jnp.where(iota((16, 16), 0) == iota((16, 16), 1), 1.0 / length[...], 0.0)
    ilc = jnp.sum(ilc, axis=1, keepdims=True)
    ilb = jnp.broadcast_to(ilc, (16, 128))
    il_kx = jnp.where(iota((16, 512), 0) == iota((16, 512), 1) >> 5, ilc, 0.0)
    il_kx = jnp.sum(il_kx, axis=0, keepdims=True)
    loads[1].wait()
    for g in range(2):
        il = il_kx[0:1, g * 256 : (g + 1) * 256]
        rows, cols = iota((16, 256), 0), iota((16, 256), 1)
        x = (cols & 31).astype(F32)
        up = jnp.exp((x - 31.0) * il)
        down = jnp.exp(-x * il) - jnp.exp((x - 2.0 * rest_x) * il)
        table = jnp.where(cols >> 5 == (rows & 7), jnp.where(rows < 8, up, down), 0.0)
        high, low = halves(table)
        for m in range(4):
            s = ctrl[m, g * 8 : (g + 1) * 8].reshape(256, 128)
            e = dot(high, s) + dot(low, s)
            lat_send[0, m, g * 8 : (g + 1) * 8, :] = e[0:8]
            lat_send[1, m, g * 8 : (g + 1) * 8, :] = e[8:16]

    pl.semaphore_wait(barrier, TILES - 1 + LAT * (Y * C - 1) + LON + 6)
    lat_copies = []
    for d in range(1, LAT):
        copy = remote(
            lat_send.at[(a + d) // LAT], lat_recv.at[d - 1], lat_s.at[d - 1], lat_r.at[d - 1],
            (mem, (a + d) % LAT, b),
        )
        copy.start()
        lat_copies.append(copy)

    for load in loads[2:5]:
        load.wait()
    t = tgt[...]
    rel = (((t >> 3) + (LAT - a)) & 3) * LON + (((t & 7) + (LON - b)) & 7)
    marks = jnp.where(iota((TILES, 512), 0) == rel, 1.0, 0.0)
    before = jnp.where(iota((512, 512), 0) < iota((512, 512), 1), 1.0, 0.0).astype(BF16)
    rank = jnp.sum(dot(marks.astype(BF16), before) * marks, axis=0, keepdims=True).astype(I32)
    slot = rel * 32 + rank
    chosen = jnp.where(iota((1024, 512), 0) == slot, 1.0, 0.0).astype(BF16)
    share = y * 8 + iota((8, 64), 0)
    level = (share >> 2) * 8 + c * 4 + (share & 3)
    own = jnp.where(iota((8, 64), 1) == level, 1.0, 0.0).astype(BF16)
    picked = dot(own, weights[...])
    place = col[...]
    r8 = iota((8, 512), 0)
    places = jnp.where(r8 == 0, (place >> 7).astype(F32), (place & 127).astype(F32))
    packed = dot_nt(jnp.concatenate([picked, places], 0).astype(BF16), chosen)
    spot = jnp.broadcast_to(packed[8:9] * 128.0 + packed[9:10], (8, 1024))
    group = iota((8, 128), 1) >> 5
    kept = group == (iota((8, 128), 0) & 3)

    def turned(v, quarters):
        return pltpu.roll(v, 32 * (quarters % 4), 1) if quarters % 4 else v

    for k in range(TILES):
        block, j = slice(k // 4 * 128, k // 4 * 128 + 128), k % 4
        tile = jnp.zeros((8, 128), F32)
        for g in range(4):
            tile = jnp.where(kept & (group == g), turned(packed[0:8, block], g - j), tile)
        into = pk_send if k else pk_recv
        into[k, 0:2, :] = jnp.sum(tile.reshape(2, 4, 128), axis=1)
        into[k, 2:3, :] = turned(spot[:, block], -j)[0:1]

    pk_copies = []
    for k in range(1, TILES):
        copy = remote(
            pk_send.at[k], pk_recv.at[k], pk_s.at[k - 1], pk_r.at[k - 1],
            (mem, (a + k // LON) % LAT, (b + k % LON) % LON),
        )
        copy.start()
        pk_copies.append(copy)

    for g in range(2):
        il = il_kx[0:1, g * 256 : (g + 1) * 256]
        rows, cols = iota((256, 256), 0), iota((256, 256), 1)
        x1, x2 = (rows & 31).astype(F32), (cols & 31).astype(F32)
        near = jnp.exp(-jnp.abs(x1 - x2) * il)
        back = jnp.exp((x1 + x2 - 2.0 * rest_x) * il)
        high, low = halves(jnp.where(rows >> 5 == cols >> 5, near - back, 0.0))
        for m in range(4):
            s = ctrl[m, g * 8 : (g + 1) * 8].reshape(256, 128)
            out = dot(high, s) + dot(low, s)
            field[g * 8 : (g + 1) * 8, m * TX : (m + 1) * TX, :] = out.reshape(8, TX, TY)

    carry_l, carry_r = [0.0] * 4, [0.0] * 4
    for d in range(1, LAT):
        lat_copies[d - 1].wait_recv()
        left = jnp.where(a >= d, 1.0, 0.0)
        wl = jnp.exp(-32.0 * (d - 1) * ilb) * left
        wr = jnp.exp(-32.0 * (LAT - 1 - d) * ilb) * (1.0 - left)
        for m in range(4):
            got = lat_recv[d - 1, m]
            carry_l[m] = carry_l[m] + wl * got
            carry_r[m] = carry_r[m] + wr * got
    x = iota((TX, TY), 0).astype(F32)
    ly = iota((8, TY), 1).astype(F32)
    row8 = iota((8, TY), 0)
    for k in range(16):
        il = ilb[k : k + 1]
        ahead = jnp.exp(-(x + 1.0) * il) - jnp.exp((x - 1.0 - 2.0 * rest_x) * il)
        behind = jnp.exp((x - 32.0) * il)
        for m in range(4):
            here = slice(m * TX, (m + 1) * TX)
            field[k, here, :] = (
                field[k, here, :] + ahead * carry_l[m][k : k + 1] + behind * carry_r[m][k : k + 1]
            )
        up = jnp.exp((ly - 127.0) * il)
        down = jnp.exp(-ly * il) - jnp.exp((ly - 2.0 * rest_y) * il)
        th, tl = halves(jnp.where(row8 == 0, up, down))
        fh, fl = halves(field[k])
        e = dot_nt(th, fh) + dot_nt(th, fl) + dot_nt(tl, fh)
        lon_send[0, k : k + 1, :] = e[0:1]
        lon_send[1, k : k + 1, :] = e[1:2]
    lon_copies = []
    for d in range(1, LON):
        copy = remote(
            lon_send.at[(b + d) // LON], lon_recv.at[d - 1], lon_s.at[d - 1], lon_r.at[d - 1],
            (mem, a, (b + d) % LON),
        )
        copy.start()
        lon_copies.append(copy)

    y1, y2 = iota((TY, TY), 0).astype(F32), iota((TY, TY), 1).astype(F32)
    for k in range(16):
        il = ilb[k : k + 1]
        nh, nl = halves(
            jnp.exp(-jnp.abs(y1 - y2) * il) - jnp.exp((y1 + y2 - 2.0 * rest_y) * il)
        )
        fh, fl = halves(field[k])
        field[k] = dot(fh, nh) + dot(fl, nh) + dot(fh, nl)

    loads[5].wait()
    half = 0.5 * ilc
    sq = half * half
    gain = half * (1.0 - sq * (1.0 / 3.0 - sq * (2.0 / 15.0 - sq * (17.0 / 315.0))))
    scaled = modes[...] * (gain * (1.0 / math.sqrt(4 * ZH * Y * C - 1)))
    spread = jnp.where(iota((512, 64), 0) >> 3 == iota((512, 64), 1), 1.0, 0.0).astype(BF16)
    widen = jnp.where(iota((16, 128), 0) == iota((16, 128), 1) >> 3, 1.0, 0.0).astype(BF16)
    diagonal = (iota((512, 128), 0) & 7) == (iota((512, 128), 1) & 7)
    mh, ml = (
        jnp.where(diagonal, dot(spread, dot_tn(part, widen).astype(BF16)), 0.0).astype(BF16)
        for part in halves(scaled)
    )

    mhh = jnp.concatenate([mh, mh], 1)

    cl, cr = 0.0, 0.0
    for d in range(1, LON):
        lon_copies[d - 1].wait_recv()
        left = jnp.where(b >= d, 1.0, 0.0)
        got = lon_recv[d - 1]
        cl = cl + (jnp.exp(-128.0 * (d - 1) * ilb) * left) * got
        cr = cr + (jnp.exp(-128.0 * (LON - 1 - d) * ilb) * (1.0 - left)) * got
    for k in range(16):
        il = ilb[k : k + 1]
        ahead = jnp.exp(-(ly + 1.0) * il) - jnp.exp((ly - 1.0 - 2.0 * rest_y) * il)
        behind = jnp.exp((ly - 128.0) * il)
        ah, al = halves(jnp.where(row8 == 0, ahead, jnp.where(row8 == 1, behind, 0.0)))
        ch, co = halves(
            jnp.where(row8 == 0, cl[k : k + 1], jnp.where(row8 == 1, cr[k : k + 1], 0.0))
        )
        field[k] = field[k] + (dot_tn(ch, ah) + dot_tn(co, ah) + dot_tn(ch, al))

    for copy in pk_copies:
        copy.wait_recv()
    share_copies = []
    for d in range(1, Y):
        copy = remote(
            pk_recv, pk_all.at[d - 1], share_s.at[d - 1], share_r.at[d - 1],
            ((zh * Y + (y + d) % Y) * C + c, a, b),
        )
        copy.start()
        share_copies.append(copy)

    loads[7].wait()
    core_copies = []
    for xb in range(4):
        acc = None
        for pair in range(2):
            rows = jnp.concatenate(
                [
                    field[:, m * TX + xb * 8 : m * TX + xb * 8 + 8, :].reshape(128, 128)
                    for m in (2 * pair, 2 * pair + 1)
                ],
                1,
            )
            fh, fl = halves(rows)
            prof = dot(mhh, jnp.concatenate([fh, fl], 0)) + dot(ml, fh)
            for n in range(2):
                p = pert[2 * pair + n, :, xb * 8 : xb * 8 + 8, :].astype(F32).reshape(512, 128)
                term = prof[:, n * 128 : n * 128 + 128] * p
                acc = term if acc is None else acc + term
        total[:, :, :, xb * 8 : xb * 8 + 8, :] = acc.reshape(8, 2, 4, 8, 128)
        part = pl.ds(xb * 8, 8)
        copy = remote(
            total.at[:, 1 - c, :, part, :], core_recv.at[:, :, part, :],
            core_s.at[xb], core_r.at[xb], (mem + 1 - 2 * c, a, b),
        )
        copy.start()
        core_copies.append(copy)

    lane = iota((8, 128), 1)
    r8 = iota((8, 128), 0)
    ends = jnp.where(
        (r8 == 0) & (lane == 0) | (r8 == 1) & (lane == 127), 1.0, 0.0
    ).astype(BF16)
    halo = []
    for p, (core, dev) in enumerate(((c, mem), (1 - c, mem + 1 - 2 * c))):
        row_send[p, 0] = total[:, core, :, TX - 1, :].reshape(32, 128)
        row_send[p, 1] = total[:, core, :, 0, :].reshape(32, 128)
        bh, bl = halves(total[:, core].reshape(1024, 128))
        edge_send[p] = (dot_nt(ends, bh) + dot_nt(ends, bl))[0:2]
        for s in range(2):
            step = 1 - 2 * s
            copy = remote(
                row_send.at[p, s], row_recv.at[p, s], row_s.at[p, s], row_r.at[p, s],
                (dev, (a + step + LAT) % LAT, b),
            )
            there, back = a + step, a - step
            halo.append((copy, (there >= 0) & (there < LAT), (back >= 0) & (back < LAT)))
        for i, da in enumerate((-1, 0, 1)):
            for j, db in enumerate((-1, 1)):
                copy = remote(
                    edge_send.at[p], edge_recv.at[p, i, j], edge_s.at[p, i, j],
                    edge_r.at[p, i, j], (dev, (a - da + LAT) % LAT, (b - db + LON) % LON),
                )
                at, bt, af, bf = a - da, b - db, a + da, b + db
                halo.append((
                    copy,
                    (at >= 0) & (at < LAT) & (bt >= 0) & (bt < LON),
                    (af >= 0) & (af < LAT) & (bf >= 0) & (bf < LON),
                ))
    for copy, sends, _ in halo:
        pl.when(sends)(copy.start)

    for copy in core_copies:
        copy.wait_recv()
    whole = total[:, c] + core_recv[...]
    red1[...] = whole.reshape(2, 4, 4, TX, TY)
    y_copies = []
    for h, half in enumerate((1 - zh, zh)):
        for d in range(1, Y):
            yp = (y + d) % Y
            n = h * (Y - 1) + d - 1
            copy = remote(
                red1.at[half, yp], y_recv.at[n], y_s.at[n], y_r.at[n],
                ((zh * Y + yp) * C + c, a, b),
            )
            copy.start()
            y_copies.append(copy)

    wh, wl = halves(whole.reshape(1024, 128))

    p_all = jnp.zeros((8, 128), F32)
    for da in range(LAT):
        got = pk_recv[da * LON : (da + 1) * LON, 2, :]
        p_all = jnp.where(group == da, turned(got, da), p_all)
    ys, xs = iota((TY, 128), 0), iota((TX, 128), 0)

    def blend(near, far, at):
        return jnp.where(at == near, 0.75, 0.0) + jnp.where(at == far, 0.25, 0.0)

    double = jnp.concatenate([wh, wl], 1)
    spots = []
    for db in range(LON):
        spot = p_all[db : db + 1].astype(I32)
        i, j = spot >> 8, spot & 255
        nx, ny = i >> 1, j >> 1
        fx, fy = nx + 2 * (i & 1) - 1, ny + 2 * (j & 1) - 1
        cols, rows = blend(ny, fy, ys).astype(BF16), blend(nx, fx, xs)
        inner = dot(double, jnp.concatenate([cols, cols], 0))
        inner = jnp.sum(inner.reshape(32, TX, 128) * rows[None], axis=1)
        around = [blend(ny, fy, -1), blend(ny, fy, TY), blend(nx, fx, -1), blend(nx, fx, TX)]
        spots.append((inner, cols, rows.astype(BF16), *around))

    for d in range(Y):
        if d:
            share_copies[d - 1].wait_recv()
        source = pk_all.at[d - 1] if d else pk_recv
        for r in range(8):
            w = jnp.zeros((8, 128), F32)
            for da in range(LAT):
                got = source[da * LON : (da + 1) * LON, r // 4, :]
                w = jnp.where(group == da, turned(got, da - r % 4), w)
            w_all[d, :, r, :] = w

    for copy, _, gets in halo:
        pl.when(gets)(copy.wait_recv)
    beyond = [halves(row_recv[0, n] + row_recv[1, n]) for n in range(2)]
    beyond = jnp.concatenate([*beyond[0], *beyond[1]], 0)
    edges = edge_recv[0] + edge_recv[1]
    z32, l32 = iota((32, 1024), 0), iota((32, 1024), 1)
    fold = jnp.where(iota((1024, TX), 0) & 31 == iota((1024, TX), 1), 1.0, 0.0).astype(BF16)

    def at_level(line, where):
        return jnp.where(where, line, 0.0)

    left, right = edges[1, 0][1:2], edges[1, 1][0:1]
    same = l32 >> 5 == z32
    beside = jnp.concatenate(
        [*halves(at_level(left, same)), *halves(at_level(right, same))], 0
    )
    beside = dot(beside, fold).astype(BF16)
    corner = [
        jnp.sum(at_level(edges[i, j][1 - j : 2 - j], l32 == z32 * 32 + x), 1, keepdims=True)
        for i, x in ((0, TX - 1), (2, 0))
        for j in range(2)
    ]
    val_copies = []
    for db in range(LON):
        inner, cols, rows, west, east, north, south = spots[db]
        ud = dot(beyond, cols)
        lr = dot(beside, rows)
        up = ud[0:32] + ud[32:64] + corner[0] * west + corner[1] * east
        down = ud[64:96] + ud[96:128] + corner[2] * west + corner[3] * east
        inner = inner + (lr[0:32] + lr[32:64]) * west + (lr[64:96] + lr[96:128]) * east
        inner = inner + up * north + down * south
        blended[db] = inner.reshape(Y, 8, 128)
        parts = [w_all[d, db] * blended[db, (y + Y - d) % Y] for d in range(Y)]
        val[db] = jnp.sum(sum(parts), axis=0, keepdims=True)
        for zo in range(ZH):
            n = zo * LON + db
            if n:
                copy = remote(
                    val.at[db], val_recv.at[n], val_s.at[n - 1], val_r.at[n - 1],
                    ((mem + zo * Y * C) % (ZH * Y * C), a, (b - db + LON) % LON),
                )
                copy.start()
                val_copies.append(copy)

    for copy in y_copies[: Y - 1]:
        copy.wait_recv()
    red2[...] = red1[1 - zh, y] + y_recv[0] + y_recv[1] + y_recv[2]
    z_copy = remote(
        red2, z_recv, z_s.at[0], z_r.at[0],
        ((mem + Y * C) % (ZH * Y * C), a, b),
    )
    z_copy.start()

    val_recv[0] = val[0]
    for copy in val_copies:
        copy.wait_recv()
    for db in range(LON):
        vsum[db : db + 1, :] = val_recv[db] + val_recv[LON + db]
    both = vsum[...]
    for da in range(LAT):
        mine = jnp.zeros((8, 128), F32)
        for g in range(4):
            mine = jnp.where(kept & (group == g), turned(both, g - da), mine)
        mine = jnp.sum(mine.reshape(2, 4, 128), axis=1)
        if da:
            last_send[da - 1] = mine
        else:
            last_send[LAT - 1] = mine
            last_recv[0] = mine
    last_copies = []
    for da in range(LAT):
        for d in range(Y * C):
            n = da * Y * C + d
            if n:
                copy = remote(
                    last_send.at[(da + LAT - 1) % LAT], last_recv.at[n],
                    last_s.at[n - 1], last_r.at[n - 1],
                    (zh * Y * C + (q + d) % (Y * C), (a + LAT - da) % LAT, b),
                )
                copy.start()
                last_copies.append(copy)
    for copy in y_copies[Y - 1 :]:
        copy.wait_recv()
    own = red1[zh, y] + y_recv[3] + y_recv[4] + y_recv[5]
    z_copy.wait_recv()
    inc_ref[...] = own + z_recv[...]
    inc_copy = pltpu.make_async_copy(inc_ref, inc_hbm, load_sem.at[9])
    inc_copy.start()
    for copy in last_copies:
        copy.wait_recv()
    table = []
    for da in range(LAT):
        block = last_recv[da * Y * C]
        for d in range(1, Y * C):
            block = block + last_recv[da * Y * C + d]
        table.append(block)
    table = jnp.concatenate(table, 0)
    marks = jnp.where(iota((8, 512), 0) == rel >> 2, 1.0, 0.0).astype(BF16)
    found = sum(dot_tn(part, marks) for part in thirds(table))
    here = iota((128, 512), 0) == (rel & 3) * 32 + rank
    equivalent = jnp.sum(jnp.where(here, found, 0.0), axis=0, keepdims=True)
    loads[6].wait()
    live = iota((1, 512), 1) < count[0]
    dep_ref[...] = jnp.where(live, innovation[...] - equivalent, 0.0)
    dep_copy = pltpu.make_async_copy(dep_ref, dep_hbm, load_sem.at[8])
    dep_copy.start()
    inc_copy.wait()
    dep_copy.wait()

    for copy in (*lat_copies, *lon_copies, *pk_copies, *core_copies, *y_copies, z_copy):
        copy.wait_send()
    for copy in (*share_copies, *val_copies, *last_copies):
        copy.wait_send()
    for copy, sends, _ in halo:
        pl.when(sends)(copy.wait_send)


def deliver(increment, departures, inc_hbm, dep_hbm, inc, dep, sems):
    pairs = ((increment, inc, inc_hbm), (departures, dep, dep_hbm))
    inward = [pltpu.make_async_copy(p[0], p[1], sems.at[n]) for n, p in enumerate(pairs)]
    outward = [pltpu.make_async_copy(p[1], p[2], sems.at[2 + n]) for n, p in enumerate(pairs)]
    for copy in inward:
        copy.start()
    for back, forth in zip(inward, outward):
        back.wait()
        forth.start()
    for copy in outward:
        copy.wait()


def per_device(
    perturbation, control, filter_length, modes, obs_weights, innovation, obs_tile,
    obs_column, obs_count,
):
    vmem = pl.BlockSpec(memory_space=pltpu.VMEM)
    hbm = pl.BlockSpec(memory_space=pltpu.HBM)
    smem = pl.BlockSpec(memory_space=pltpu.SMEM)
    f32 = lambda *shape: pltpu.VMEM(shape, F32)
    sem = lambda *shape: pltpu.SemaphoreType.DMA(shape)
    pairs = lambda *shape: [sem(*shape), sem(*shape)]
    increment, departures = pl.pallas_call(
        kernel,
        out_shape=(
            jax.ShapeDtypeStruct((4, TX, TY), F32),
            jax.ShapeDtypeStruct((1, 512), F32),
        ),
        in_specs=[hbm] * 6 + [smem] + [hbm] * 2,
        out_specs=(hbm, hbm),
        scratch_shapes=[
            f32(1, 16), f32(16, 64), pltpu.VMEM((64, 512), BF16), f32(1, 512),
            pltpu.VMEM((1, 512), I32), pltpu.VMEM((1, 512), I32),
            pltpu.VMEM((4, 16, TX, TY), BF16), pltpu.VMEM((4, 64, TX, TY), BF16),
            f32(16, 128, TY),
            f32(2, 4, 16, TY), f32(LAT - 1, 4, 16, TY),
            f32(2, 16, 128), f32(LON - 1, 16, 128),
            f32(TILES, 3, 128), f32(TILES, 3, 128),
            f32(Y - 1, TILES, 3, 128), f32(Y, LON, 8, 128), f32(LON, Y, 8, 128),
            f32(8, 2, 4, TX, TY), f32(8, 4, TX, TY),
            f32(2, 4, 4, TX, TY), f32(2 * (Y - 1), 4, TX, TY),
            f32(4, TX, TY), f32(4, TX, TY),
            f32(2, 2, 32, 128), f32(2, 2, 32, 128), f32(2, 2, 1024), f32(2, 3, 2, 2, 1024),
            f32(LON, 1, 128), f32(ZH * LON, 1, 128), f32(8, 128),
            f32(LAT, 2, 128), f32(LAT * Y * C, 2, 128),
            f32(4, TX, TY), f32(1, 512),
            sem(10), *pairs(LAT - 1), *pairs(LON - 1), *pairs(TILES - 1),
            *pairs(Y - 1), *pairs(4),
            *pairs(2 * (Y - 1)), *pairs(1), *pairs(2, 2), *pairs(2, 3, 2), *pairs(ZH * LON - 1),
            *pairs(LAT * Y * C - 1),
        ],
        compiler_params=pltpu.CompilerParams(
            collective_id=0, has_side_effects=True, vmem_limit_bytes=60_000_000
        ),
        name="hybrid",
    )(
        filter_length.reshape(1, 16),
        modes.T,
        obs_weights.T,
        innovation.reshape(1, 512),
        obs_tile.reshape(1, 512),
        obs_column.reshape(1, 512),
        obs_count,
        control,
        perturbation,
    )
    increment, departures = pl.pallas_call(
        deliver,
        out_shape=(
            jax.ShapeDtypeStruct((4, TX, TY), F32),
            jax.ShapeDtypeStruct((1, 512), F32),
        ),
        in_specs=[hbm] * 2,
        out_specs=(hbm, hbm),
        scratch_shapes=[f32(4, TX, TY), f32(1, 512), sem(4)],
        name="deliver",
    )(increment, departures)
    return increment, departures.reshape(512)


def solution(mesh):
    placed = (
        P("mem", None, "lat", "lon"),
        P("mem", None, "lat", "lon"),
        P(),
        P(),
        P(("lat", "lon"), None),
        P(("lat", "lon")),
        P(("lat", "lon"), None),
        P(("lat", "lon")),
        P(("lat", "lon")),
    )
    return jax.shard_map(
        per_device,
        mesh=mesh,
        in_specs=placed,
        out_specs=(P("mem", "lat", "lon"), P(("lat", "lon"))),
        check_vma=False,
    )
```
